32 devices in a mesh: rep: 2 (over x), tp: 4 (over z), dp: 4 (over y, core).
Axes of the slice: x: 2, y: 2, z: 4, core: 2. Of those that a mesh axis runs over, the one named last changes fastest.
Arguments:
- grad_partial: float32 [8, 4, 1024, 4096], P(('rep', 'dp'), None, None, 'tp'), parts along dimension 0
- momentum: float32 [8, 1024, 4096], P('rep', 'dp', 'tp'), parts along dimension 0
- weight: float32 [8, 1024, 4096], P('rep', 'dp', 'tp'), parts along dimension 0
- learn_rate: float32 [8], P('rep'), parts along dimension 0
- decay_rate: float32 [], replicated
Outputs:
- output 1: float32 [8, 1024, 4096], P('rep', 'dp', 'tp'), parts along dimension 0
- output 2: float32 [8, 1024, 4096], P('rep', 'dp', 'tp'), parts along dimension 0
- output 3: bfloat16 [8, 1024, 4096], P('rep', None, 'tp'), parts along dimension 0
There are 2 independent parts. The reference program is written for one: setup_inputs(seed, part) draws one part's arguments, and reference() takes and returns one part's arrays. A program takes and returns all parts, laid end to end along the dimension named above; an argument that names none is the same for every part.
All inputs are finite; a program needn't handle non-finite values.
Results may differ from the reference program's by a relative error of at most 0.0110385.
Values are sent between devices in bfloat16 or wider.
A program may use at most 1 GiB of HBM per device.

```python
import math
import jax
import jax.numpy as jnp
from jax import lax

DP_SIZE = 4
MATS = 4
ROWS = 1024
COLS = 4096

MOMENTUM = 0.95
NS_STEPS = 5
COEF_A = 3.4445
COEF_B = -4.7750
COEF_C = 2.0315
NORM_EPS = 1e-7
OUT_SCALE = 0.2 * math.sqrt(max(ROWS, COLS))


def setup_inputs(seed: int = 0, part: int = 0) -> dict:
    part_key = jax.random.fold_in(jax.random.key(seed), part)
    key_grad, key_scale, key_mom, key_weight, key_rate = jax.random.split(part_key, 5)
    key_decay = jax.random.key(seed + 1)
    dev_scale = jax.random.uniform(key_scale, (DP_SIZE, 1, 1, 1), minval=0.5, maxval=2.0)
    grad_partial = jax.random.normal(key_grad, (DP_SIZE, MATS, ROWS, COLS)) * dev_scale * math.sqrt(DP_SIZE)
    momentum = jax.random.normal(key_mom, (MATS, ROWS, COLS))
    weight = 0.25 * jax.random.normal(key_weight, (MATS, ROWS, COLS))
    learn_rate = jax.random.uniform(key_rate, (MATS,), minval=0.1, maxval=1.0)
    decay_rate = jax.random.uniform(key_decay, (), minval=0.2, maxval=0.5)
    return {
        "grad_partial": grad_partial.astype(jnp.float32),
        "momentum": momentum.astype(jnp.float32),
        "weight": weight.astype(jnp.float32),
        "learn_rate": learn_rate.astype(jnp.float32),
        "decay_rate": decay_rate.astype(jnp.float32),
    }


def orthogonalize(update):
    upd_f32 = update.astype(jnp.float32)
    norm_val = jnp.sqrt(jnp.sum(upd_f32 * upd_f32))
    x_cur = (upd_f32 / (norm_val + NORM_EPS)).astype(jnp.bfloat16)
    if ROWS > COLS:
        x_cur = x_cur.T
    for step_idx in range(NS_STEPS):
        gram_mat = jnp.dot(x_cur, x_cur.T, preferred_element_type=jnp.float32).astype(jnp.bfloat16)
        gram_sq = jnp.dot(gram_mat, gram_mat, preferred_element_type=jnp.float32)
        poly_mat = (COEF_B * gram_mat.astype(jnp.float32) + COEF_C * gram_sq).astype(jnp.bfloat16)
        prod_mat = jnp.dot(poly_mat, x_cur, preferred_element_type=jnp.float32)
        x_cur = (COEF_A * x_cur.astype(jnp.float32) + prod_mat).astype(jnp.bfloat16)
    if ROWS > COLS:
        x_cur = x_cur.T
    return x_cur


def reference(grad_partial, momentum, weight, learn_rate, decay_rate):
    grad_mean = jnp.mean(grad_partial, axis=0)
    mom_new = MOMENTUM * momentum + grad_mean
    update = (grad_mean + MOMENTUM * mom_new).astype(jnp.bfloat16)
    ortho_mat = lax.map(orthogonalize, update)
    rate_col = learn_rate[:, None, None]
    weight_new = weight - rate_col * (OUT_SCALE * ortho_mat.astype(jnp.float32) + decay_rate * weight)
    return mom_new, weight_new, weight_new.astype(jnp.bfloat16)
```

```python
import functools
import math

import jax
import jax.numpy as jnp
from jax import lax
from jax.experimental import pallas as pl
from jax.experimental.pallas import tpu as pltpu
from jax.sharding import PartitionSpec as P

MOMENTUM = 0.95
NS_STEPS = 5
COEF_A = 3.4445
COEF_B = -4.7750
COEF_C = 2.0315
NORM_EPS = 1e-7

MATS = 4
DP = 4
TP = 4
HALVES = 2
F32 = jnp.float32
BF16 = jnp.bfloat16
NT = (((1,), (1,)), ((), ()))

ORDER = [(0, 0), (2, 0), (0, 1), (2, 1), (1, 0), (3, 0), (1, 1), (3, 1)]


def mesh_copy(src, dst, send, recv, **axes):
    return pltpu.make_async_remote_copy(
        src_ref=src, dst_ref=dst, send_sem=send, recv_sem=recv,
        device_id=axes, device_id_type=pl.DeviceIdType.MESH)


def relations():
    me = lax.axis_index("dp")
    y, c = lax.div(me, 2), lax.rem(me, 2)
    return me, 2 * y + (1 - c), 2 * (1 - y) + c, 2 * (1 - y) + (1 - c)


def front_kernel(grad, mom, mom_new, ub_out,
                 own_yp, own_me, recv_a, recv_b, recv_y, momb, ub, xg,
                 ld_yp, ld_me, ld_mom, sa, ra, sb, rb, sy, ry, su, ru, zr, zsr, zsl, so, sm):
    me, partner, yp, diag = relations()
    z = lax.axis_index("tp")
    nchunk = len(ORDER)
    half = own_me.shape[1]
    rows = HALVES * half

    barrier = pltpu.get_barrier_semaphore()
    for peer in (partner, yp, diag):
        pl.semaphore_signal(barrier, inc=1, device_id={"dp": peer}, device_id_type=pl.DeviceIdType.MESH)

    @pl.when(z > 0)
    def _():
        pl.semaphore_signal(barrier, inc=1, device_id={"tp": z - 1}, device_id_type=pl.DeviceIdType.MESH)

    @pl.when(z < TP - 1)
    def _():
        pl.semaphore_signal(barrier, inc=1, device_id={"tp": z + 1}, device_id_type=pl.DeviceIdType.MESH)

    def load_yp(k):
        m, h = ORDER[k]
        return pltpu.make_async_copy(grad.at[0, m, pl.ds(yp * rows + h * half, half), :], own_yp.at[k], ld_yp.at[k])

    def load_me(k):
        m, h = ORDER[k]
        return pltpu.make_async_copy(grad.at[0, m, pl.ds(me * rows + h * half, half), :], own_me.at[k], ld_me.at[k])

    def load_mom(k):
        m, h = ORDER[k]
        return pltpu.make_async_copy(mom.at[m, pl.ds(h * half, half), :], momb.at[k], ld_mom.at[k])

    def copy_a(k):
        m, h = ORDER[k]
        return mesh_copy(grad.at[0, m, pl.ds(diag * rows + h * half, half), :], recv_a.at[k], sa.at[k], ra.at[k], dp=partner)

    def copy_b(k):
        m, h = ORDER[k]
        return mesh_copy(grad.at[0, m, pl.ds(partner * rows + h * half, half), :], recv_b.at[k], sb.at[k], rb.at[k], dp=partner)

    def copy_y(k):
        return mesh_copy(own_yp.at[k], recv_y.at[k], sy.at[k], ry.at[k], dp=yp)

    def store_mom(k):
        m, h = ORDER[k]
        return pltpu.make_async_copy(momb.at[k], mom_new.at[m, pl.ds(h * half, half), :], sm.at[k])

    def chunk_rows(r, h):
        return pl.ds(pl.multiple_of(r * rows + h * half, half), half)

    def copy_u(k):
        m, h = ORDER[k]
        return mesh_copy(ub.at[k], xg.at[z, chunk_rows(me, h), :], su.at[k], ru.at[me, h], dp=m)

    for k in range(nchunk):
        load_yp(k).start()
    for k in range(nchunk):
        load_me(k).start()
        load_mom(k).start()
    pl.semaphore_wait(barrier, 3 + jnp.where(z > 0, 1, 0) + jnp.where(z < TP - 1, 1, 0))
    for k in range(nchunk):
        copy_a(k).start()
    for k in range(nchunk):
        copy_b(k).start()

    def chip_sum(k):
        load_yp(k).wait()
        copy_a(k).wait_recv()

        @pl.loop(0, half // 32)
        def _(i):
            sl = pl.ds(pl.multiple_of(i * 32, 32), 32)
            own_yp[k, sl, :] = own_yp[k, sl, :] + recv_a[k, sl, :]

    def update_chunk(k):
        m, h = ORDER[k]
        load_me(k).wait()
        copy_b(k).wait_recv()
        load_mom(k).wait()
        copy_y(k).wait_recv()

        @pl.loop(0, half // 32)
        def _(i):
            sl = pl.ds(pl.multiple_of(i * 32, 32), 32)
            g = (own_me[k, sl, :] + recv_b[k, sl, :] + recv_y[k, sl, :]) * (1.0 / DP)
            mn = MOMENTUM * momb[k, sl, :] + g
            momb[k, sl, :] = mn
            ub[k, sl, :] = (g + MOMENTUM * mn).astype(BF16)

        @pl.when(me == m)
        def _():
            xg[z, chunk_rows(m, h), :] = ub[k]

        @pl.when(me != m)
        def _():
            copy_u(k).start()

        store_mom(k).start()

    chunks = [(h, i) for h in range(HALVES) for i in range(DP)]
    peer_of = (me, partner, yp, diag)

    def z_rows(q):
        h, i = chunks[q]
        return chunk_rows(peer_of[i], h)

    def z_right(q, s):
        return mesh_copy(xg.at[s, z_rows(q), :], xg.at[s, z_rows(q), :], zsr.at[s, q], zr.at[s, q], tp=z + 1)

    def z_left(q, s):
        return mesh_copy(xg.at[s, z_rows(q), :], xg.at[s, z_rows(q), :], zsl.at[s, q], zr.at[s, q], tp=z - 1)

    def z_out(q, s):
        return pltpu.make_async_copy(xg.at[s, z_rows(q), :], ub_out.at[s, z_rows(q), :], so.at[s, q])

    def z_own(q):
        h, i = chunks[q]
        if i > 0:
            r = peer_of[i]
            mesh_copy(ub.at[0], xg.at[z, chunk_rows(r, h), :], su.at[0], ru.at[r, h], dp=r).wait_recv()

        @pl.when(z < TP - 1)
        def _():
            z_right(q, z).start()

        @pl.when(z > 0)
        def _():
            z_left(q, z).start()

        z_out(q, z).start()

    def z_forward(q, step):
        @pl.when(z - step >= 0)
        def _():
            z_left(q, z - step).wait_recv()

            @pl.when(z < TP - 1)
            def _():
                z_right(q, z - step).start()

            z_out(q, z - step).start()

        @pl.when(z + step < TP)
        def _():
            z_left(q, z + step).wait_recv()

            @pl.when(z > 0)
            def _():
                z_left(q, z + step).start()

            z_out(q, z + step).start()

    def z_stage(t):
        nq = len(chunks)
        if t < nq:
            z_own(t)
        for step in range(1, TP):
            if 0 <= t - step < nq:
                z_forward(t - step, step)

    early = {1: (0, 1), 2: (2, 3), 3: (4, 5), 4: (6, 7), 5: (8, 9, 10)}
    late = {5: (0, 1), 6: (2, 3), 7: (4, 5, 6, 7, 8, 9, 10)}

    chip_sum(0)
    chip_sum(1)
    copy_y(0).start()
    copy_y(1).start()
    for k in range(nchunk):
        if k + 2 < nchunk:
            chip_sum(k + 2)
        update_chunk(k)
        if k + 2 < nchunk:
            copy_y(k + 2).start()
        if k in early:
            @pl.when(lax.rem(me, 2) == 0)
            def _():
                for t in early[k]:
                    z_stage(t)
        if k in late:
            @pl.when(lax.rem(me, 2) == 1)
            def _():
                for t in late[k]:
                    z_stage(t)

    for k in range(nchunk):
        copy_a(k).wait_send()
        copy_b(k).wait_send()
        copy_y(k).wait_send()
        store_mom(k).wait()

        @pl.when(me != ORDER[k][0])
        def _():
            copy_u(k).wait_send()
    for q in range(len(chunks)):
        for s in range(TP):
            z_out(q, s).wait()

            @pl.when(jnp.logical_and(s <= z, z < TP - 1))
            def _():
                z_right(q, s).wait_send()

            @pl.when(jnp.logical_and(s >= z, z > 0))
            def _():
                z_left(q, s).wait_send()


def front(grad, mom):
    _, mats, all_rows, cols = grad.shape
    rows = mom.shape[1]
    half = rows // HALVES
    n = len(ORDER)
    dma = pltpu.SemaphoreType.DMA
    buf = pltpu.VMEM((n, half, cols), F32)
    return pl.pallas_call(
        front_kernel,
        out_shape=(jax.ShapeDtypeStruct(mom.shape, F32), jax.ShapeDtypeStruct((TP, all_rows, cols), BF16)),
        in_specs=[pl.BlockSpec(memory_space=pl.ANY)] * 2,
        out_specs=[pl.BlockSpec(memory_space=pl.ANY)] * 2,
        scratch_shapes=[buf] * 6 + [pltpu.VMEM((n, half, cols), BF16), pltpu.VMEM((TP, all_rows, cols), BF16)]
        + [dma((n,))] * 10 + [dma((DP, HALVES))] + [dma((TP, n))] * 4 + [dma((n,))],
        compiler_params=pltpu.CompilerParams(collective_id=0, has_side_effects=True, vmem_limit_bytes=60 * 2**20),
        name="front",
    )(grad, mom)


def dot(a, b):
    return jnp.dot(a, b, preferred_element_type=F32)


def ortho_kernel(u, out, x, gram, poly):
    size, width = x.shape
    part = width // TP
    block = 256
    nblk = size // block

    def square_sum(i, acc):
        sl = pl.ds(pl.multiple_of(i * 16, 16), 16)
        for s in range(TP):
            v = u[s, sl, :].astype(F32)
            acc = acc + v * v
        return acc

    total = lax.fori_loop(0, size // 16, square_sum, jnp.zeros((16, part), F32))
    inv = 1.0 / (jnp.sqrt(jnp.sum(total, keepdims=True)) + NORM_EPS)

    @pl.loop(0, size // 16)
    def _(i):
        sl = pl.ds(pl.multiple_of(i * 16, 16), 16)
        for s in range(TP):
            x[sl, s * part:(s + 1) * part] = (u[s, sl, :].astype(F32) * inv).astype(BF16)

    def make_poly():
        for i in range(nblk):
            for j in range(i, nblk):
                blk = lax.dot_general(x[i * block:(i + 1) * block, :], x[j * block:(j + 1) * block, :], NT,
                                      preferred_element_type=F32).astype(BF16)
                gram[i * block:(i + 1) * block, j * block:(j + 1) * block] = blk
                if j > i:
                    gram[j * block:(j + 1) * block, i * block:(i + 1) * block] = blk.T
        poly[...] = (COEF_B * gram[...].astype(F32) + COEF_C * dot(gram[...], gram[...])).astype(BF16)

    @pl.loop(0, NS_STEPS - 1)
    def _(step):
        make_poly()

        @pl.loop(0, TP)
        def _(t):
            cs = pl.ds(pl.multiple_of(t * part, part), part)
            xc = x[:, cs]
            x[:, cs] = (COEF_A * xc.astype(F32) + dot(poly[...], xc)).astype(BF16)

    make_poly()
    xc = x[:, pl.ds(pl.multiple_of(lax.axis_index("tp") * part, part), part)]
    out[...] = (COEF_A * xc.astype(F32) + dot(poly[...], xc)).astype(BF16)


def ortho(ub):
    tp, size, part = ub.shape
    width = tp * part
    flops = 2 * size * size * (2 * width + size) * NS_STEPS
    return pl.pallas_call(
        ortho_kernel,
        out_shape=jax.ShapeDtypeStruct((size, part), BF16),
        in_specs=[pl.BlockSpec(memory_space=pltpu.VMEM)],
        out_specs=pl.BlockSpec(memory_space=pltpu.VMEM),
        scratch_shapes=[pltpu.VMEM((size, width), BF16), pltpu.VMEM((size, size), BF16), pltpu.VMEM((size, size), BF16)],
        compiler_params=pltpu.CompilerParams(vmem_limit_bytes=56 * 2**20),
        cost_estimate=pl.CostEstimate(flops=flops, bytes_accessed=2 * size * width, transcendentals=0),
        name="ortho",
    )(ub)


def tail_kernel(out_scale, x5, wg_p, wg_yp, wg_diag, weight, lr, decay,
                w_new, wb,
                xv, wgv, wv, xr, ws, wo, wn,
                lx, lg, lw, sx, rx, sw, swy, ry, rd, sd, sf, sl_b, sl_n):
    me, partner, yp, diag = relations()
    rows = weight.shape[1]
    peers = (me, partner, yp, diag)

    barrier = pltpu.get_barrier_semaphore()
    for peer in peers[1:]:
        pl.semaphore_signal(barrier, inc=1, device_id={"dp": peer}, device_id_type=pl.DeviceIdType.MESH)

    def block(r):
        return pl.ds(pl.multiple_of(r * rows, rows), rows)

    load_g = [pltpu.make_async_copy(ref, wgv.at[i], lg.at[i]) for i, ref in enumerate((wg_p, wg_yp, wg_diag))]
    load_x = [pltpu.make_async_copy(x5.at[block(peers[i]), :], xv.at[i], lx.at[i]) for i in range(DP)]
    load_w = [pltpu.make_async_copy(weight.at[peers[i]], wv.at[i], lw.at[i]) for i in range(DP)]
    for c in load_x + load_w + load_g:
        c.start()
    pl.semaphore_wait(barrier, 3)

    send_x = [mesh_copy(x5.at[block(peers[i]), :], xr.at[me], sx.at[i], rx.at[me], dp=peers[i]) for i in range(1, DP)]
    for c in (send_x[1], send_x[2], send_x[0]):
        c.start()

    def apply(w, x, mat):
        return w - lr[mat] * (out_scale * x.astype(F32) + decay[0] * w)

    def each(fn):
        @pl.loop(0, rows // 32)
        def _(i):
            fn(pl.ds(pl.multiple_of(i * 32, 32), 32))

    def to_partner(src, mat, r, sem):
        return mesh_copy(src, wb.at[mat, block(r), :], sem, rd.at[mat, r], dp=partner)

    local_b = []
    own_sends = []
    for i in range(DP):
        load_x[i].wait()
        if i == 0:
            load_w[0].wait()

            def own(sl):
                w = apply(wv[0, sl, :], xv[0, sl, :], me)
                wn[0, sl, :] = w
                ws[0, sl, :] = w.astype(BF16)
            each(own)
            c = pltpu.make_async_copy(wn.at[0], w_new.at[me], sl_n.at[0])
            c.start()
            local_b.append(c)
        else:
            load_g[i - 1].wait()

            def other(sl, i=i):
                ws[i, sl, :] = apply(wgv[i - 1, sl, :], xv[i, sl, :], me).astype(BF16)
            each(other)
        if i < 2:
            c = mesh_copy(ws.at[i], wb.at[me, block(peers[i]), :], swy.at[i], ry.at[me], dp=peers[2 + i])
            c.start()
            own_sends.append(c)
        if i != 1:
            c = to_partner(ws.at[i], me, peers[i], sd.at[i])
            c.start()
            own_sends.append(c)
        c = pltpu.make_async_copy(ws.at[i], wb.at[me, block(peers[i]), :], sl_b.at[i])
        c.start()
        local_b.append(c)

    for i in range(1, DP):
        load_w[i].wait()
        mesh_copy(x5.at[block(me), :], xr.at[peers[i]], sx.at[0], rx.at[peers[i]], dp=peers[i]).wait_recv()

        def rest(sl, i=i):
            w = apply(wv[i, sl, :], xr[peers[i], sl, :], peers[i])
            wn[i, sl, :] = w
            wo[i, sl, :] = w.astype(BF16)
        each(rest)
        if i > 1:
            c = to_partner(wo.at[i], peers[i], me, sw.at[i])
            c.start()
            own_sends.append(c)
        for c in (pltpu.make_async_copy(wn.at[i], w_new.at[peers[i]], sl_n.at[i]),
                  pltpu.make_async_copy(wo.at[i], wb.at[peers[i], block(me), :], sl_b.at[DP + i])):
            c.start()
            local_b.append(c)

    for i in (2, 3):
        dst = wb.at[peers[i], block(yp), :]
        mesh_copy(ws.at[0], dst, swy.at[0], ry.at[peers[i]], dp=peers[i]).wait_recv()
        c = to_partner(dst, peers[i], yp, sf.at[i])
        c.start()
        own_sends.append(c)

    for mat, r in ((partner, partner), (partner, yp), (partner, diag), (yp, partner), (diag, partner), (yp, diag), (diag, diag)):
        to_partner(ws.at[0], mat, r, sd.at[0]).wait_recv()
    for c in send_x + own_sends:
        c.wait_send()
    for c in local_b:
        c.wait()


def tail(x5, wg, weight, lr, decay, out_scale):
    mats, rows, cols = weight.shape
    all_rows = DP * rows
    dma = pltpu.SemaphoreType.DMA
    hbm = pl.BlockSpec(memory_space=pl.ANY)
    smem = pl.BlockSpec(memory_space=pltpu.SMEM)
    b16 = pltpu.VMEM((DP, rows, cols), BF16)
    f32 = pltpu.VMEM((DP, rows, cols), F32)
    return pl.pallas_call(
        functools.partial(tail_kernel, out_scale),
        out_shape=(jax.ShapeDtypeStruct(weight.shape, F32), jax.ShapeDtypeStruct((mats, all_rows, cols), BF16)),
        in_specs=[hbm] * 5 + [smem] * 2,
        out_specs=[hbm] * 2,
        scratch_shapes=[b16, pltpu.VMEM((DP - 1, rows, cols), F32), f32, b16, b16, b16, f32,
                        dma((DP,)), dma((DP - 1,)), dma((DP,)), dma((DP,)), dma((DP,)), dma((DP,)), dma((2,)), dma((DP,)),
                        dma((DP, DP)), dma((DP,)), dma((DP,)), dma((2 * DP,)), dma((DP,))],
        compiler_params=pltpu.CompilerParams(collective_id=1, has_side_effects=True, vmem_limit_bytes=60 * 2**20),
        name="tail",
    )(x5, *wg, weight, lr, decay)


def solution(mesh):
    def local_step(grad, mom, weight, learn_rate, decay_rate):
        mom_new, ub = front(grad, mom)
        weight_late, ub = lax.optimization_barrier((weight, ub))
        me = lax.axis_index("dp")
        y, c = me // 2, me % 2
        pairs = (
            (2 * y + (1 - c), [(0, 1), (1, 0), (2, 3), (3, 2)]),
            (2 * (1 - y) + c, [(0, 2), (2, 0), (1, 3), (3, 1)]),
            (2 * (1 - y) + (1 - c), [(0, 3), (3, 0), (1, 2), (2, 1)]),
        )
        wg = [lax.ppermute(lax.dynamic_index_in_dim(weight_late, peer, 0, keepdims=False), "dp", perm)
              for peer, perm in pairs]
        x5 = ortho(ub)
        out_scale = 0.2 * math.sqrt(max(grad.shape[2], grad.shape[3] * TP))
        weight_new, weight_full = tail(x5, wg, weight, learn_rate, decay_rate.reshape(1), out_scale)
        return mom_new, weight_new, weight_full

    return jax.shard_map(
        local_step,
        mesh=mesh,
        in_specs=(P(("rep", "dp"), None, None, "tp"), P("rep", "dp", "tp"), P("rep", "dp", "tp"), P("rep"), P()),
        out_specs=(P("rep", "dp", "tp"), P("rep", "dp", "tp"), P("rep", None, "tp")),
        check_vma=False,
    )
```

```python
import functools
import math

import jax
import jax.numpy as jnp
from jax import lax
from jax.experimental import pallas as pl
from jax.experimental.pallas import tpu as pltpu
from jax.sharding import PartitionSpec as P

MOMENTUM = 0.95
NS_STEPS = 5
COEF_A = 3.4445
COEF_B = -4.7750
COEF_C = 2.0315
NORM_EPS = 1e-7

DP = 4
TP = 4
F32 = jnp.float32
BF16 = jnp.bfloat16
NT = (((1,), (1,)), ((), ()))

ORDER = [(0, 0), (2, 0), (0, 1), (2, 1), (1, 0), (3, 0), (1, 1), (3, 1), (1, 2), (3, 2)]
PARTS = {0: [(0, 32), (32, 32)], 1: [(0, 32), (32, 16), (48, 16)]}
MAX_PARTS = 3
STAGES = {
    0: {1: (0, 1), 2: (2, 3), 3: (4, 5), 4: (6, 7), 5: (8,)},
    1: {5: (0, 1), 6: (2, 3), 7: (4, 5), 8: (6, 7), 9: (8, 9, 10, 11, 12)},
}
STEP = 32


def mesh_copy(src, dst, send, recv, **axes):
    return pltpu.make_async_remote_copy(
        src_ref=src, dst_ref=dst, send_sem=send, recv_sem=recv,
        device_id=axes, device_id_type=pl.DeviceIdType.MESH)


def dot(a, b):
    return jnp.dot(a, b, preferred_element_type=F32)


def muon_kernel(out_scale, grad, mom, weight, lr, decay,
                mom_new, w_new, wb,
                own_yp, own_me, recv_a, recv_b, recv_y, momb, ub, x, gram, poly, x5, x5e, wg, xr, ws, wo,
                ld_yp, ld_me, ld_mom, sa, ra, sb, rb, sy, ry, su, sm, ru,
                zs, zf, zr, pw, rw, lw, se, re, sx, rx, sw, rwb, sd, rd, sf, sl_b, sl_n):
    me = lax.axis_index("dp")
    z = lax.axis_index("tp")
    y, c = lax.div(me, 2), lax.rem(me, 2)
    partner, yp, diag = 2 * y + (1 - c), 2 * (1 - y) + c, 2 * (1 - y) + (1 - c)
    peers = (me, partner, yp, diag)
    rows, cols = mom.shape[1], mom.shape[2]
    unit = rows // 64
    npiece = len(ORDER)
    middle = jnp.logical_and(z > 0, z < TP - 1)
    left = z < TP // 2
    nb = jnp.where(left, z + 1, z - 1)
    other = TP - 1 - z
    end = jnp.where(left, 0, TP - 1)
    far = TP - 1 - end

    barrier = pltpu.get_barrier_semaphore()
    for peer in peers[1:]:
        pl.semaphore_signal(barrier, inc=1, device_id={"dp": peer}, device_id_type=pl.DeviceIdType.MESH)

    @pl.when(z > 0)
    def _():
        pl.semaphore_signal(barrier, inc=1, device_id={"tp": z - 1}, device_id_type=pl.DeviceIdType.MESH)

    @pl.when(z < TP - 1)
    def _():
        pl.semaphore_signal(barrier, inc=1, device_id={"tp": z + 1}, device_id_type=pl.DeviceIdType.MESH)

    def span(k):
        m, p = ORDER[k]
        lo, n = PARTS[m % 2][p]
        return m, p, lo * unit, n * unit

    def grad_rows(r, k):
        m, _, lo, n = span(k)
        return grad.at[0, m, pl.ds(pl.multiple_of(r * rows + lo, 16), n), :]

    def piece(buf, k):
        m, _, lo, n = span(k)
        return buf.at[m, pl.ds(lo, n), :]

    def load_yp(k):
        return pltpu.make_async_copy(grad_rows(yp, k), piece(own_yp, k), ld_yp.at[k])

    def load_me(k):
        return pltpu.make_async_copy(grad_rows(me, k), piece(own_me, k), ld_me.at[k])

    def load_mom(k):
        return pltpu.make_async_copy(piece(mom, k), piece(momb, k), ld_mom.at[k])

    def copy_a(k):
        return mesh_copy(grad_rows(diag, k), piece(recv_a, k), sa.at[k], ra.at[k], dp=partner)

    def copy_b(k):
        return mesh_copy(grad_rows(partner, k), piece(recv_b, k), sb.at[k], rb.at[k], dp=partner)

    def copy_y(k):
        return mesh_copy(piece(own_yp, k), piece(recv_y, k), sy.at[k], ry.at[k], dp=yp)

    def store_mom(k):
        return pltpu.make_async_copy(piece(momb, k), piece(mom_new, k), sm.at[k])

    def x_block(r, lo, n, s):
        return x.at[pl.ds(pl.multiple_of(r * rows + lo, 16), n), pl.ds(pl.multiple_of(s * cols, cols), cols)]

    def copy_u(k):
        m, p, lo, n = span(k)
        return mesh_copy(piece(ub, k), x_block(me, lo, n, z), su.at[k], ru.at[me, p], dp=m)

    for k in range(npiece):
        load_yp(k).start()
    for k in range(npiece):
        load_me(k).start()
        load_mom(k).start()
    pl.semaphore_wait(barrier, 3 + jnp.where(z > 0, 1, 0) + jnp.where(z < TP - 1, 1, 0))
    for k in range(npiece):
        copy_a(k).start()
    for k in range(npiece):
        copy_b(k).start()

    def chip_sum(k):
        m, _, lo, n = span(k)
        load_yp(k).wait()
        copy_a(k).wait_recv()

        @pl.loop(0, n // STEP)
        def _(i):
            sl = pl.ds(pl.multiple_of(lo + i * STEP, STEP), STEP)
            own_yp[m, sl, :] = own_yp[m, sl, :] + recv_a[m, sl, :]

    def update_piece(k):
        m, _, lo, n = span(k)
        load_me(k).wait()
        copy_b(k).wait_recv()
        load_mom(k).wait()
        copy_y(k).wait_recv()

        @pl.loop(0, n // STEP)
        def _(i):
            sl = pl.ds(pl.multiple_of(lo + i * STEP, STEP), STEP)
            g = (own_me[m, sl, :] + recv_b[m, sl, :] + recv_y[m, sl, :]) * (1.0 / DP)
            mn = MOMENTUM * momb[m, sl, :] + g
            momb[m, sl, :] = mn
            ub[m, sl, :] = (g + MOMENTUM * mn).astype(BF16)

        @pl.when(me == m)
        def _():
            x[pl.ds(pl.multiple_of(me * rows + lo, 16), n), pl.ds(pl.multiple_of(z * cols, cols), cols)] = ub[m, lo:lo + n, :]

        @pl.when(me != m)
        def _():
            copy_u(k).start()

        store_mom(k).start()

    def gather(core):
        todo = [(p, lo * unit, n * unit, i) for p, (lo, n) in enumerate(PARTS[core]) for i in range(DP)]

        def copy_own(q):
            _, lo, n, i = todo[q]
            blk = x_block(peers[i], lo, n, z)
            return mesh_copy(blk, blk, zs.at[q], zr.at[z, q], tp=nb)

        def copy_on(q):
            _, lo, n, i = todo[q]
            blk = x_block(peers[i], lo, n, end)
            return mesh_copy(blk, blk, zf.at[q], zr.at[end, q], tp=other)

        def landed(q, s):
            _, lo, n, i = todo[q]
            blk = x_block(peers[i], lo, n, s)
            mesh_copy(blk, blk, zs.at[q], zr.at[s, q], tp=nb).wait_recv()

        def stage(t):
            if t < len(todo):
                p, lo, n, i = todo[t]
                if i > 0:
                    mesh_copy(ub.at[0, pl.ds(0, n), :], x_block(peers[i], lo, n, z), su.at[0], ru.at[peers[i], p],
                              dp=peers[i]).wait_recv()
                copy_own(t).start()
            if t > 0:
                @pl.when(middle)
                def _():
                    landed(t - 1, end)
                    copy_on(t - 1).start()

        def finish():
            for q in range(len(todo)):
                @pl.when(middle)
                def _():
                    landed(q, other)
                    landed(q, far)

        def drain():
            for q in range(len(todo)):
                copy_own(q).wait_send()

                @pl.when(middle)
                def _():
                    copy_on(q).wait_send()

        return stage, finish, drain

    gathers = [gather(0), gather(1)]

    def on_core(core, fn):
        @pl.when(c == core)
        def _():
            fn()

    chip_sum(0)
    chip_sum(1)
    copy_y(0).start()
    copy_y(1).start()
    for k in range(npiece):
        if k + 2 < npiece:
            chip_sum(k + 2)
        update_piece(k)
        if k + 2 < npiece:
            copy_y(k + 2).start()
        for core in range(2):
            if k in STAGES[core]:
                on_core(core, lambda: [gathers[core][0](t) for t in STAGES[core][k]])
    for core in range(2):
        on_core(core, gathers[core][1])
        on_core(core, gathers[core][2])

    def copy_w(i):
        return mesh_copy(weight.at[peers[i]], wg.at[i - 1], pw.at[i], rw.at[i], dp=peers[i])

    wv = own_me
    load_w = [pltpu.make_async_copy(weight.at[peers[i]], wv.at[i], lw.at[i]) for i in range(DP)]
    for i in range(1, DP):
        copy_w(i).start()
    for cp in load_w:
        cp.start()

    size, width = x.shape
    block = 256
    nblk = size // block

    def column(s):
        return pl.ds(pl.multiple_of(s * cols, cols), cols)

    def row_block(r):
        return pl.ds(pl.multiple_of(r * rows, rows), rows)

    def make_poly():
        for i in range(nblk):
            for j in range(i, nblk):
                blk = lax.dot_general(x[i * block:(i + 1) * block, :], x[j * block:(j + 1) * block, :], NT,
                                      preferred_element_type=F32).astype(BF16)
                gram[i * block:(i + 1) * block, j * block:(j + 1) * block] = blk
                if j > i:
                    gram[j * block:(j + 1) * block, i * block:(i + 1) * block] = blk.T
        poly[...] = (COEF_B * gram[...].astype(F32) + COEF_C * dot(gram[...], gram[...])).astype(BF16)

    @pl.when(middle)
    def _():
        def square_sum(i, acc):
            v = x[pl.ds(pl.multiple_of(i * 16, 16), 16), :].astype(F32)
            return acc + v * v

        total = lax.fori_loop(0, size // 16, square_sum, jnp.zeros((16, width), F32))
        inv = 1.0 / (jnp.sqrt(jnp.sum(total, keepdims=True)) + NORM_EPS)

        @pl.loop(0, size // 16)
        def _(i):
            sl = pl.ds(pl.multiple_of(i * 16, 16), 16)
            x[sl, :] = (x[sl, :].astype(F32) * inv).astype(BF16)

        @pl.loop(0, NS_STEPS)
        def _(step):
            make_poly()

            @pl.when(step < NS_STEPS - 1)
            def _():
                @pl.loop(0, TP)
                def _(t):
                    cs = column(t)
                    xc = x[:, cs]
                    x[:, cs] = (COEF_A * xc.astype(F32) + dot(poly[...], xc)).astype(BF16)

    def copy_e(i):
        blk = row_block(peers[i])
        return mesh_copy(x5e.at[blk, :], x5.at[blk, :], se.at[i], re.at[i], tp=end)

    def last(i, s, dst):
        blk = row_block(peers[i])
        dst[blk, :] = (COEF_A * x[blk, column(s)].astype(F32) + dot(poly[blk, :], x[:, column(s)])).astype(BF16)

    def apply(w, v, mat):
        return w - lr[mat] * (out_scale * v.astype(F32) + decay[0] * w)

    def each(fn):
        @pl.loop(0, rows // STEP)
        def _(i):
            fn(pl.ds(pl.multiple_of(i * STEP, STEP), STEP))

    def to_partner(src, mat, r, sem):
        return mesh_copy(src, wb.at[mat, row_block(r), :], sem, rd.at[mat, r], dp=partner)

    sends = []
    stores = []

    def go(cp, into):
        cp.start()
        into.append(cp)

    for i in (2, 3, 0, 1):
        r = peers[i]

        @pl.when(middle)
        def _():
            last(i, end, x5e)
            copy_e(i).start()
            last(i, z, x5)

        @pl.when(jnp.logical_not(middle))
        def _():
            copy_e(i).wait_recv()

        if i > 0:
            go(mesh_copy(x5.at[row_block(r), :], xr.at[me], sx.at[i], rx.at[me], dp=r), sends)
        if i == 0:
            load_w[0].wait()

            def own(sl):
                w = apply(wv[0, sl, :], x5[pl.ds(me * rows + sl.start, STEP), :], me)
                wv[0, sl, :] = w
                ws[0, sl, :] = w.astype(BF16)
            each(own)
            go(pltpu.make_async_copy(wv.at[0], w_new.at[me], sl_n.at[0]), stores)
        else:
            copy_w(i).wait_recv()

            def rest(sl, i=i, r=r):
                ws[i, sl, :] = apply(wg[i - 1, sl, :], x5[pl.ds(r * rows + sl.start, STEP), :], me).astype(BF16)
            each(rest)
        if i < 2:
            go(mesh_copy(ws.at[i], wb.at[me, row_block(r), :], sw.at[i], rwb.at[me], dp=peers[2 + i]), sends)
        if i != 1:
            go(to_partner(ws.at[i], me, r, sd.at[i]), sends)
        go(pltpu.make_async_copy(ws.at[i], wb.at[me, row_block(r), :], sl_b.at[i]), stores)

    for i in range(1, DP):
        mat = peers[i]
        load_w[i].wait()
        mesh_copy(x5.at[row_block(me), :], xr.at[mat], sx.at[0], rx.at[mat], dp=mat).wait_recv()

        def mine(sl, i=i, mat=mat):
            w = apply(wv[i, sl, :], xr[mat, sl, :], mat)
            wv[i, sl, :] = w
            wo[i, sl, :] = w.astype(BF16)
        each(mine)
        if i > 1:
            go(to_partner(wo.at[i], mat, me, sf.at[i]), sends)
        go(pltpu.make_async_copy(wv.at[i], w_new.at[mat], sl_n.at[i]), stores)
        go(pltpu.make_async_copy(wo.at[i], wb.at[mat, row_block(me), :], sl_b.at[DP + i]), stores)

    for i in (2, 3):
        dst = wb.at[peers[i], row_block(yp), :]
        mesh_copy(ws.at[0], dst, sw.at[0], rwb.at[peers[i]], dp=peers[i]).wait_recv()
        go(to_partner(dst, peers[i], yp, sf.at[DP + i]), sends)

    for mat, r in ((partner, partner), (partner, yp), (partner, diag), (yp, partner), (diag, partner), (yp, diag), (diag, diag)):
        to_partner(ws.at[0], mat, r, sd.at[0]).wait_recv()

    for k in range(npiece):
        copy_a(k).wait_send()
        copy_b(k).wait_send()
        copy_y(k).wait_send()
        store_mom(k).wait()

        @pl.when(me != ORDER[k][0])
        def _():
            copy_u(k).wait_send()
    for i in range(DP):
        if i > 0:
            copy_w(i).wait_send()

        @pl.when(middle)
        def _():
            copy_e(i).wait_send()
    for cp in sends:
        cp.wait_send()
    for cp in stores:
        cp.wait()


def muon(grad, mom, weight, lr, decay, out_scale):
    _, mats, all_rows, cols = grad.shape
    rows = mom.shape[1]
    n = len(ORDER)
    nq = DP * MAX_PARTS
    dma = pltpu.SemaphoreType.DMA
    hbm = pl.BlockSpec(memory_space=pl.ANY)
    smem = pl.BlockSpec(memory_space=pltpu.SMEM)
    f32 = pltpu.VMEM((mats, rows, cols), F32)
    b16 = pltpu.VMEM((mats, rows, cols), BF16)
    square = pltpu.VMEM((all_rows, all_rows), BF16)
    slab = pltpu.VMEM((all_rows, cols), BF16)
    return pl.pallas_call(
        functools.partial(muon_kernel, out_scale),
        out_shape=(jax.ShapeDtypeStruct(mom.shape, F32), jax.ShapeDtypeStruct(weight.shape, F32),
                   jax.ShapeDtypeStruct((mats, all_rows, cols), BF16)),
        in_specs=[hbm] * 3 + [smem] * 2,
        out_specs=[hbm] * 3,
        scratch_shapes=[f32] * 6 + [b16, pltpu.VMEM((all_rows, TP * cols), BF16), square, square, slab, slab,
                                    pltpu.VMEM((DP - 1, rows, cols), F32), b16, b16, b16]
        + [dma((n,))] * 11 + [dma((DP, MAX_PARTS)), dma((nq,)), dma((nq,)), dma((TP, nq))]
        + [dma((DP,))] * 9 + [dma((DP,)), dma((DP, DP)), dma((2 * DP,)), dma((2 * DP,)), dma((DP,))],
        compiler_params=pltpu.CompilerParams(collective_id=0, has_side_effects=True, vmem_limit_bytes=67043328),
        name="muon",
    )(grad, mom, weight, lr, decay)


def solution(mesh):
    def local_step(grad, mom, weight, learn_rate, decay_rate):
        out_scale = 0.2 * math.sqrt(max(grad.shape[2], grad.shape[3] * TP))
        return muon(grad, mom, weight, learn_rate, decay_rate.reshape(1), out_scale)

    return jax.shard_map(
        local_step,
        mesh=mesh,
        in_specs=(P(("rep", "dp"), None, None, "tp"), P("rep", "dp", "tp"), P("rep", "dp", "tp"), P("rep"), P()),
        out_specs=(P("rep", "dp", "tp"), P("rep", "dp", "tp"), P("rep", None, "tp")),
        check_vma=False,
    )
```

```python
import functools
import math

import jax
import jax.numpy as jnp
from jax import lax
from jax.experimental import pallas as pl
from jax.experimental.pallas import tpu as pltpu
from jax.sharding import PartitionSpec as P

MOMENTUM = 0.95
NS_STEPS = 5
COEF_A = 3.4445
COEF_B = -4.7750
COEF_C = 2.0315
NORM_EPS = 1e-7

DP = 4
TP = 4
F32 = jnp.float32
BF16 = jnp.bfloat16
NT = (((1,), (1,)), ((), ()))

ORDER = [(0, 0), (2, 0), (0, 1), (2, 1), (1, 0), (3, 0), (1, 1), (3, 1), (1, 2), (3, 2), (1, 3), (3, 3)]
PARTS = {0: [(0, 32), (32, 32)], 1: [(0, 32), (32, 16), (48, 8), (56, 8)]}
MAX_PARTS = 4
SENT = [3, 4, 5, 6, 7, 8, 9, 10, 12, 12, 12, 12]
STAGES = {
    (0, 0): {0: (0, 1), 1: (2, 3), 2: (4, 5), 3: (6, 7), 4: (8,)},
    (0, 1): {1: (0, 1), 2: (2, 3), 3: (4, 5), 4: (6, 7), 5: (8,)},
    (1, 0): {4: (0, 1), 5: (2, 3), 6: (4, 5), 7: (6, 7), 8: (8, 9), 9: (10, 11), 10: (12, 13), 11: (14, 15, 16)},
    (1, 1): {5: (0, 1), 6: (2, 3), 7: (4, 5), 8: (6, 7), 9: (8, 9), 10: (10, 11), 11: (12, 13, 14, 15, 16)},
}
HEAD = 5
STEP = 32


def mesh_copy(src, dst, send, recv, **axes):
    return pltpu.make_async_remote_copy(
        src_ref=src, dst_ref=dst, send_sem=send, recv_sem=recv,
        device_id=axes, device_id_type=pl.DeviceIdType.MESH)


def dot(a, b):
    return jnp.dot(a, b, preferred_element_type=F32)


def muon_kernel(out_scale, grad, mom, weight, lr, decay,
                mom_new, w_new, wb,
                own_yp, own_me, recv_a, recv_b, recv_y, momb, ub, x, gram, poly, x5, x5e, wg, xr, ws, wo, ssq,
                ld_yp, ld_me, ld_mom, sa, ra, sb, rb, sy, ry, su, sm, ru,
                zs, zf, zr, pw, rw, lw, se, re, sx, rx, sw, rwb, sd, rd, sf, sl_b, sl_n):
    me = lax.axis_index("dp")
    z = lax.axis_index("tp")
    y, c = lax.div(me, 2), lax.rem(me, 2)
    partner, yp, diag = 2 * y + (1 - c), 2 * (1 - y) + c, 2 * (1 - y) + (1 - c)
    peers = (me, partner, yp, diag)
    rows, cols = mom.shape[1], mom.shape[2]
    unit = rows // 64
    npiece = len(ORDER)
    middle = jnp.logical_and(z > 0, z < TP - 1)
    left = z < TP // 2
    nb = jnp.where(left, z + 1, z - 1)
    other = TP - 1 - z
    end = jnp.where(left, 0, TP - 1)
    far = TP - 1 - end

    barrier = pltpu.get_barrier_semaphore()
    for peer in peers[1:]:
        pl.semaphore_signal(barrier, inc=1, device_id={"dp": peer}, device_id_type=pl.DeviceIdType.MESH)

    @pl.when(z > 0)
    def _():
        pl.semaphore_signal(barrier, inc=1, device_id={"tp": z - 1}, device_id_type=pl.DeviceIdType.MESH)

    @pl.when(z < TP - 1)
    def _():
        pl.semaphore_signal(barrier, inc=1, device_id={"tp": z + 1}, device_id_type=pl.DeviceIdType.MESH)

    def span(k):
        m, p = ORDER[k]
        lo, n = PARTS[m % 2][p]
        return m, p, lo * unit, n * unit

    def grad_rows(r, k):
        m, _, lo, n = span(k)
        return grad.at[0, m, pl.ds(pl.multiple_of(r * rows + lo, 16), n), :]

    def piece(buf, k):
        m, _, lo, n = span(k)
        return buf.at[m, pl.ds(lo, n), :]

    def load_yp(k):
        return pltpu.make_async_copy(grad_rows(yp, k), piece(own_yp, k), ld_yp.at[k])

    def load_me(k):
        return pltpu.make_async_copy(grad_rows(me, k), piece(own_me, k), ld_me.at[k])

    def load_mom(k):
        return pltpu.make_async_copy(piece(mom, k), piece(momb, k), ld_mom.at[k])

    def copy_a(k):
        return mesh_copy(grad_rows(diag, k), piece(recv_a, k), sa.at[k], ra.at[k], dp=partner)

    def copy_b(k):
        return mesh_copy(grad_rows(partner, k), piece(recv_b, k), sb.at[k], rb.at[k], dp=partner)

    def copy_y(k):
        return mesh_copy(piece(own_yp, k), piece(recv_y, k), sy.at[k], ry.at[k], dp=yp)

    def store_mom(k):
        return pltpu.make_async_copy(piece(momb, k), piece(mom_new, k), sm.at[k])

    def x_block(r, lo, n, s):
        return x.at[pl.ds(pl.multiple_of(r * rows + lo, 16), n), pl.ds(pl.multiple_of(s * cols, cols), cols)]

    def copy_u(k):
        m, p, lo, n = span(k)
        return mesh_copy(piece(ub, k), x_block(me, lo, n, z), su.at[k], ru.at[me, p], dp=m)

    for k in range(npiece):
        load_yp(k).start()
    for k in range(npiece):
        load_me(k).start()
        load_mom(k).start()
    pl.semaphore_wait(barrier, 3 + jnp.where(z > 0, 1, 0) + jnp.where(z < TP - 1, 1, 0))
    for k in range(npiece):
        copy_a(k).start()
    for k in range(npiece):
        copy_b(k).start()

    def chip_sum(k):
        m, _, lo, n = span(k)
        load_yp(k).wait()
        copy_a(k).wait_recv()

        @pl.loop(0, n // STEP)
        def _(i):
            sl = pl.ds(pl.multiple_of(lo + i * STEP, STEP), STEP)
            own_yp[m, sl, :] = own_yp[m, sl, :] + recv_a[m, sl, :]

    def update_piece(k):
        m, _, lo, n = span(k)
        load_me(k).wait()
        copy_b(k).wait_recv()
        load_mom(k).wait()
        copy_y(k).wait_recv()

        @pl.loop(0, n // STEP)
        def _(i):
            sl = pl.ds(pl.multiple_of(lo + i * STEP, STEP), STEP)
            g = (own_me[m, sl, :] + recv_b[m, sl, :] + recv_y[m, sl, :]) * (1.0 / DP)
            mn = MOMENTUM * momb[m, sl, :] + g
            momb[m, sl, :] = mn
            ub[m, sl, :] = (g + MOMENTUM * mn).astype(BF16)

        @pl.when(me == m)
        def _():
            x[pl.ds(pl.multiple_of(me * rows + lo, 16), n), pl.ds(pl.multiple_of(z * cols, cols), cols)] = ub[m, lo:lo + n, :]

        @pl.when(me != m)
        def _():
            copy_u(k).start()

        store_mom(k).start()

    def gather(core):
        todo = [(p, lo * unit, n * unit, i) for p, (lo, n) in enumerate(PARTS[core]) for i in range(DP)]

        def copy_own(q):
            _, lo, n, i = todo[q]
            blk = x_block(peers[i], lo, n, z)
            return mesh_copy(blk, blk, zs.at[q], zr.at[z, q], tp=nb)

        def copy_on(q):
            _, lo, n, i = todo[q]
            blk = x_block(peers[i], lo, n, end)
            return mesh_copy(blk, blk, zf.at[q], zr.at[end, q], tp=other)

        def landed(q, s):
            _, lo, n, i = todo[q]
            blk = x_block(peers[i], lo, n, s)
            mesh_copy(blk, blk, zs.at[q], zr.at[s, q], tp=nb).wait_recv()

        def stage(t):
            if t < len(todo):
                p, lo, n, i = todo[t]
                if i > 0:
                    mesh_copy(ub.at[0, pl.ds(0, n), :], x_block(peers[i], lo, n, z), su.at[0], ru.at[peers[i], p],
                              dp=peers[i]).wait_recv()
                copy_own(t).start()
            if t > 0:
                @pl.when(middle)
                def _():
                    landed(t - 1, end)
                    copy_on(t - 1).start()

        def finish():
            for q in range(len(todo)):
                @pl.when(middle)
                def _():
                    landed(q, other)
                    landed(q, far)
                    _, lo, n, i = todo[q]
                    base = peers[i] * rows + lo

                    def square_sum(t, acc):
                        v = x[pl.ds(pl.multiple_of(base + t * 16, 16), 16), :].astype(F32)
                        return acc + v * v

                    part = lax.fori_loop(0, n // 16, square_sum, jnp.zeros(ssq.shape, F32))
                    ssq[...] = part if q == 0 else ssq[...] + part

        def drain():
            for q in range(len(todo)):
                copy_own(q).wait_send()

                @pl.when(middle)
                def _():
                    copy_on(q).wait_send()

        return stage, finish, drain

    gathers = [gather(0), gather(1)]

    def on_core(core, fn):
        @pl.when(c == core)
        def _():
            fn()

    size, width = x.shape
    block = 256
    nblk = size // block

    def column(s):
        return pl.ds(pl.multiple_of(s * cols, cols), cols)

    def row_block(r):
        return pl.ds(pl.multiple_of(r * rows, rows), rows)

    def normalize():
        inv = 1.0 / (jnp.sqrt(jnp.sum(ssq[...], keepdims=True)) + NORM_EPS)

        @pl.loop(0, size // 16)
        def _(i):
            sl = pl.ds(pl.multiple_of(i * 16, 16), 16)
            x[sl, :] = (x[sl, :].astype(F32) * inv).astype(BF16)

    def square():
        for i in range(nblk):
            for j in range(i, nblk):
                blk = lax.dot_general(x[i * block:(i + 1) * block, :], x[j * block:(j + 1) * block, :], NT,
                                      preferred_element_type=F32).astype(BF16)
                gram[i * block:(i + 1) * block, j * block:(j + 1) * block] = blk
                if j > i:
                    gram[j * block:(j + 1) * block, i * block:(i + 1) * block] = blk.T

    def polynomial():
        for i in range(nblk):
            ra, rb = i * block, (i + 1) * block
            strip = (COEF_B * gram[ra:rb, ra:].astype(F32) + COEF_C * dot(gram[ra:rb, :], gram[:, ra:])).astype(BF16)
            poly[ra:rb, ra:] = strip
            for j in range(i + 1, nblk):
                poly[j * block:(j + 1) * block, ra:rb] = strip[:, j * block - ra:(j + 1) * block - ra].T

    def update(lo, hi):
        @pl.loop(lo, hi)
        def _(t):
            cs = column(t)
            xc = x[:, cs]
            x[:, cs] = (COEF_A * xc.astype(F32) + dot(poly[...], xc)).astype(BF16)

    def in_middle(fn):
        @pl.when(middle)
        def _():
            fn()

    def head(k):
        if k == HEAD:
            gathers[0][1]()
            gathers[0][2]()

            def begin():
                normalize()
                square()
            in_middle(begin)
        if k == HEAD + 1:
            in_middle(polynomial)
        if k == HEAD + 2:
            in_middle(lambda: update(0, TP // 2))
        if k == npiece - 1:
            in_middle(lambda: update(TP // 2, TP))

    chip_sum(0)
    chip_sum(1)
    copy_y(0).start()
    copy_y(1).start()
    sent = 2
    for k in range(npiece):
        for j in range(sent, SENT[k]):
            chip_sum(j)
        update_piece(k)
        for j in range(sent, SENT[k]):
            copy_y(j).start()
        sent = SENT[k]
        for (core, chip), stages in STAGES.items():
            if k in stages:
                @pl.when(jnp.logical_and(c == core, y == chip))
                def _():
                    for t in stages[k]:
                        gathers[core][0](t)
        if k in (HEAD, HEAD + 1, HEAD + 2):
            on_core(0, lambda: head(k))

    def copy_w(i):
        return mesh_copy(weight.at[peers[i]], wg.at[i - 1], pw.at[i], rw.at[i], dp=peers[i])

    wv = own_me
    load_w = [pltpu.make_async_copy(weight.at[peers[i]], wv.at[i], lw.at[i]) for i in range(DP)]
    for i in range(1, DP):
        copy_w(i).start()
    for cp in load_w:
        cp.start()

    on_core(0, lambda: head(npiece - 1))

    def catch_up():
        gathers[1][1]()
        gathers[1][2]()
        in_middle(normalize)
    on_core(1, catch_up)

    @pl.when(middle)
    def _():
        def step(i, carry):
            square()
            polynomial()

            @pl.when(i < NS_STEPS - 1)
            def _():
                update(0, TP)
            return carry
        lax.fori_loop(1 - c, NS_STEPS, step, 0)

    def copy_e(i):
        blk = row_block(peers[i])
        return mesh_copy(x5e.at[blk, :], x5.at[blk, :], se.at[i], re.at[i], tp=end)

    def last(i, s, dst):
        blk = row_block(peers[i])
        dst[blk, :] = (COEF_A * x[blk, column(s)].astype(F32) + dot(poly[blk, :], x[:, column(s)])).astype(BF16)

    def apply(w, v, mat):
        return w - lr[mat] * (out_scale * v.astype(F32) + decay[0] * w)

    def each(fn):
        @pl.loop(0, rows // STEP)
        def _(i):
            fn(pl.ds(pl.multiple_of(i * STEP, STEP), STEP))

    def to_partner(src, mat, r, sem):
        return mesh_copy(src, wb.at[mat, row_block(r), :], sem, rd.at[mat, r], dp=partner)

    sends = []
    stores = []

    def go(cp, into):
        cp.start()
        into.append(cp)

    for i in (2, 3, 0, 1):
        r = peers[i]

        @pl.when(middle)
        def _():
            last(i, end, x5e)
            copy_e(i).start()
            last(i, z, x5)

        @pl.when(jnp.logical_not(middle))
        def _():
            copy_e(i).wait_recv()

        if i > 0:
            go(mesh_copy(x5.at[row_block(r), :], xr.at[me], sx.at[i], rx.at[me], dp=r), sends)
        if i == 0:
            load_w[0].wait()

            def own(sl):
                w = apply(wv[0, sl, :], x5[pl.ds(me * rows + sl.start, STEP), :], me)
                wv[0, sl, :] = w
                ws[0, sl, :] = w.astype(BF16)
            each(own)
            go(pltpu.make_async_copy(wv.at[0], w_new.at[me], sl_n.at[0]), stores)
        else:
            copy_w(i).wait_recv()

            def rest(sl, i=i, r=r):
                ws[i, sl, :] = apply(wg[i - 1, sl, :], x5[pl.ds(r * rows + sl.start, STEP), :], me).astype(BF16)
            each(rest)
        if i < 2:
            go(mesh_copy(ws.at[i], wb.at[me, row_block(r), :], sw.at[i], rwb.at[me], dp=peers[2 + i]), sends)
        if i != 1:
            go(to_partner(ws.at[i], me, r, sd.at[i]), sends)
        go(pltpu.make_async_copy(ws.at[i], wb.at[me, row_block(r), :], sl_b.at[i]), stores)

    for i in range(1, DP):
        mat = peers[i]
        load_w[i].wait()
        mesh_copy(x5.at[row_block(me), :], xr.at[mat], sx.at[0], rx.at[mat], dp=mat).wait_recv()

        def mine(sl, i=i, mat=mat):
            w = apply(wv[i, sl, :], xr[mat, sl, :], mat)
            wv[i, sl, :] = w
            wo[i, sl, :] = w.astype(BF16)
        each(mine)
        if i > 1:
            go(to_partner(wo.at[i], mat, me, sf.at[i]), sends)
        go(pltpu.make_async_copy(wv.at[i], w_new.at[mat], sl_n.at[i]), stores)
        go(pltpu.make_async_copy(wo.at[i], wb.at[mat, row_block(me), :], sl_b.at[DP + i]), stores)

    for i in (2, 3):
        dst = wb.at[peers[i], row_block(yp), :]
        mesh_copy(ws.at[0], dst, sw.at[0], rwb.at[peers[i]], dp=peers[i]).wait_recv()
        go(to_partner(dst, peers[i], yp, sf.at[DP + i]), sends)

    for mat, r in ((partner, partner), (partner, yp), (partner, diag), (yp, partner), (diag, partner), (yp, diag), (diag, diag)):
        to_partner(ws.at[0], mat, r, sd.at[0]).wait_recv()

    for k in range(npiece):
        copy_a(k).wait_send()
        copy_b(k).wait_send()
        copy_y(k).wait_send()
        store_mom(k).wait()

        @pl.when(me != ORDER[k][0])
        def _():
            copy_u(k).wait_send()
    for i in range(DP):
        if i > 0:
            copy_w(i).wait_send()

        @pl.when(middle)
        def _():
            copy_e(i).wait_send()
    for cp in sends:
        cp.wait_send()
    for cp in stores:
        cp.wait()


def muon(grad, mom, weight, lr, decay, out_scale):
    _, mats, all_rows, cols = grad.shape
    rows = mom.shape[1]
    n = len(ORDER)
    nq = DP * MAX_PARTS
    dma = pltpu.SemaphoreType.DMA
    hbm = pl.BlockSpec(memory_space=pl.ANY)
    smem = pl.BlockSpec(memory_space=pltpu.SMEM)
    f32 = pltpu.VMEM((mats, rows, cols), F32)
    b16 = pltpu.VMEM((mats, rows, cols), BF16)
    square = pltpu.VMEM((all_rows, all_rows), BF16)
    slab = pltpu.VMEM((all_rows, cols), BF16)
    return pl.pallas_call(
        functools.partial(muon_kernel, out_scale),
        out_shape=(jax.ShapeDtypeStruct(mom.shape, F32), jax.ShapeDtypeStruct(weight.shape, F32),
                   jax.ShapeDtypeStruct((mats, all_rows, cols), BF16)),
        in_specs=[hbm] * 3 + [smem] * 2,
        out_specs=[hbm] * 3,
        scratch_shapes=[f32] * 6 + [b16, pltpu.VMEM((all_rows, TP * cols), BF16), square, square, slab, slab,
                                    pltpu.VMEM((DP - 1, rows, cols), F32), b16, b16, b16, pltpu.VMEM((16, TP * cols), F32)]
        + [dma((n,))] * 11 + [dma((DP, MAX_PARTS)), dma((nq,)), dma((nq,)), dma((TP, nq))]
        + [dma((DP,))] * 9 + [dma((DP,)), dma((DP, DP)), dma((2 * DP,)), dma((2 * DP,)), dma((DP,))],
        compiler_params=pltpu.CompilerParams(collective_id=0, has_side_effects=True, vmem_limit_bytes=67043328),
        name="muon",
    )(grad, mom, weight, lr, decay)


def solution(mesh):
    def local_step(grad, mom, weight, learn_rate, decay_rate):
        out_scale = 0.2 * math.sqrt(max(grad.shape[2], grad.shape[3] * TP))
        return muon(grad, mom, weight, learn_rate, decay_rate.reshape(1), out_scale)

    return jax.shard_map(
        local_step,
        mesh=mesh,
        in_specs=(P(("rep", "dp"), None, None, "tp"), P("rep", "dp", "tp"), P("rep", "dp", "tp"), P("rep"), P()),
        out_specs=(P("rep", "dp", "tp"), P("rep", "dp", "tp"), P("rep", None, "tp")),
        check_vma=False,
    )
```

```python
import functools
import math

import jax
import jax.numpy as jnp
from jax import lax
from jax.experimental import pallas as pl
from jax.experimental.pallas import tpu as pltpu
from jax.sharding import PartitionSpec as P

MOMENTUM = 0.95
NS_STEPS = 5
COEF_A = 3.4445
COEF_B = -4.7750
COEF_C = 2.0315
NORM_EPS = 1e-7

DP = 4
TP = 4
F32 = jnp.float32
BF16 = jnp.bfloat16
NT = (((1,), (1,)), ((), ()))

ORDER = [(m, p) for p in range(4) for m in (0, 2)] + [(m, p) for p in range(5) for m in (1, 3)]
PARTS = {0: [(0, 16), (16, 16), (32, 16), (48, 16)], 1: [(0, 16), (16, 16), (32, 16), (48, 8), (56, 8)]}
MAX_PARTS = 5
NPIECE = len(ORDER)
SENT = [k + 3 if k < 14 else NPIECE for k in range(NPIECE)]


def stages(core, chip):
    first, parts = (0, 4) if core == 0 else (8, 5)
    out = {}
    for p in range(parts):
        k = first + 2 * p + chip
        out.setdefault(k, []).extend((4 * p, 4 * p + 1))
        out.setdefault(min(k + 1, NPIECE - 1), []).extend((4 * p + 2, 4 * p + 3))
    out.setdefault(min(k + 2, NPIECE - 1), []).append(4 * parts)
    return out


STAGES = {(core, chip): stages(core, chip) for core in range(2) for chip in range(2)}
HEAD = 9
STEP = 32


def mesh_copy(src, dst, send, recv, **axes):
    return pltpu.make_async_remote_copy(
        src_ref=src, dst_ref=dst, send_sem=send, recv_sem=recv,
        device_id=axes, device_id_type=pl.DeviceIdType.MESH)


def dot(a, b):
    return jnp.dot(a, b, preferred_element_type=F32)


def muon_kernel(out_scale, grad, mom, weight, lr, decay,
                mom_new, w_new, wb,
                own_yp, own_me, recv_a, recv_b, recv_y, momb, ub, x, gram, poly, x5, x5e, wg, xr, ws, wo, ssq,
                ld_yp, ld_me, ld_mom, sa, ra, sb, rb, sy, ry, su, sm, ru,
                zs, zf, zr, pw, rw, lw, se, re, sx, rx, sw, rwb, sd, sm2, sf, sl_b, sl_o, sl_n, rd):
    me = lax.axis_index("dp")
    z = lax.axis_index("tp")
    y, c = lax.div(me, 2), lax.rem(me, 2)
    partner, yp, diag = 2 * y + (1 - c), 2 * (1 - y) + c, 2 * (1 - y) + (1 - c)
    peers = (me, partner, yp, diag)
    rows, cols = mom.shape[1], mom.shape[2]
    unit = rows // 64
    npiece = len(ORDER)
    middle = jnp.logical_and(z > 0, z < TP - 1)
    left = z < TP // 2
    nb = jnp.where(left, z + 1, z - 1)
    other = TP - 1 - z
    end = jnp.where(left, 0, TP - 1)
    far = TP - 1 - end

    barrier = pltpu.get_barrier_semaphore()
    for peer in peers[1:]:
        pl.semaphore_signal(barrier, inc=1, device_id={"dp": peer}, device_id_type=pl.DeviceIdType.MESH)

    @pl.when(z > 0)
    def _():
        pl.semaphore_signal(barrier, inc=1, device_id={"tp": z - 1}, device_id_type=pl.DeviceIdType.MESH)

    @pl.when(z < TP - 1)
    def _():
        pl.semaphore_signal(barrier, inc=1, device_id={"tp": z + 1}, device_id_type=pl.DeviceIdType.MESH)

    def span(k):
        m, p = ORDER[k]
        lo, n = PARTS[m % 2][p]
        return m, p, lo * unit, n * unit

    def grad_rows(r, k):
        m, _, lo, n = span(k)
        return grad.at[0, m, pl.ds(pl.multiple_of(r * rows + lo, 16), n), :]

    def piece(buf, k):
        m, _, lo, n = span(k)
        return buf.at[m, pl.ds(lo, n), :]

    def load_yp(k):
        return pltpu.make_async_copy(grad_rows(yp, k), piece(own_yp, k), ld_yp.at[k])

    def load_me(k):
        return pltpu.make_async_copy(grad_rows(me, k), piece(own_me, k), ld_me.at[k])

    def load_mom(k):
        return pltpu.make_async_copy(piece(mom, k), piece(momb, k), ld_mom.at[k])

    def copy_a(k):
        return mesh_copy(grad_rows(diag, k), piece(recv_a, k), sa.at[k], ra.at[k], dp=partner)

    def copy_b(k):
        return mesh_copy(grad_rows(partner, k), piece(recv_b, k), sb.at[k], rb.at[k], dp=partner)

    def copy_y(k):
        return mesh_copy(piece(own_yp, k), piece(recv_y, k), sy.at[k], ry.at[k], dp=yp)

    def store_mom(k):
        return pltpu.make_async_copy(piece(momb, k), piece(mom_new, k), sm.at[k])

    def x_block(r, lo, n, s):
        return x.at[pl.ds(pl.multiple_of(r * rows + lo, 16), n), pl.ds(pl.multiple_of(s * cols, cols), cols)]

    def copy_u(k):
        m, p, lo, n = span(k)
        return mesh_copy(piece(ub, k), x_block(me, lo, n, z), su.at[k], ru.at[me, p], dp=m)

    for k in range(npiece):
        load_yp(k).start()
    for k in range(npiece):
        load_me(k).start()
        load_mom(k).start()
    pl.semaphore_wait(barrier, 3 + jnp.where(z > 0, 1, 0) + jnp.where(z < TP - 1, 1, 0))
    for k in range(npiece):
        copy_a(k).start()
    for k in range(npiece):
        copy_b(k).start()

    def chip_sum(k):
        m, _, lo, n = span(k)
        load_yp(k).wait()
        copy_a(k).wait_recv()

        @pl.loop(0, n // STEP)
        def _(i):
            sl = pl.ds(pl.multiple_of(lo + i * STEP, STEP), STEP)
            own_yp[m, sl, :] = own_yp[m, sl, :] + recv_a[m, sl, :]

    def update_piece(k):
        m, _, lo, n = span(k)
        load_me(k).wait()
        copy_b(k).wait_recv()
        load_mom(k).wait()
        copy_y(k).wait_recv()

        @pl.loop(0, n // STEP)
        def _(i):
            sl = pl.ds(pl.multiple_of(lo + i * STEP, STEP), STEP)
            g = (own_me[m, sl, :] + recv_b[m, sl, :] + recv_y[m, sl, :]) * (1.0 / DP)
            mn = MOMENTUM * momb[m, sl, :] + g
            momb[m, sl, :] = mn
            ub[m, sl, :] = (g + MOMENTUM * mn).astype(BF16)

        @pl.when(me == m)
        def _():
            x[pl.ds(pl.multiple_of(me * rows + lo, 16), n), pl.ds(pl.multiple_of(z * cols, cols), cols)] = ub[m, lo:lo + n, :]

        @pl.when(me != m)
        def _():
            copy_u(k).start()

        store_mom(k).start()

    def gather(core):
        todo = [(p, lo * unit, n * unit, i) for p, (lo, n) in enumerate(PARTS[core]) for i in range(DP)]

        def copy_own(q):
            _, lo, n, i = todo[q]
            blk = x_block(peers[i], lo, n, z)
            return mesh_copy(blk, blk, zs.at[q], zr.at[z, q], tp=nb)

        def copy_on(q):
            _, lo, n, i = todo[q]
            blk = x_block(peers[i], lo, n, end)
            return mesh_copy(blk, blk, zf.at[q], zr.at[end, q], tp=other)

        def landed(q, s):
            _, lo, n, i = todo[q]
            blk = x_block(peers[i], lo, n, s)
            mesh_copy(blk, blk, zs.at[q], zr.at[s, q], tp=nb).wait_recv()

        def stage(t):
            if t < len(todo):
                p, lo, n, i = todo[t]
                if i > 0:
                    mesh_copy(ub.at[0, pl.ds(0, n), :], x_block(peers[i], lo, n, z), su.at[0], ru.at[peers[i], p],
                              dp=peers[i]).wait_recv()
                copy_own(t).start()
            if t > 0:
                @pl.when(middle)
                def _():
                    landed(t - 1, end)
                    copy_on(t - 1).start()

        def finish():
            for q in range(len(todo)):
                @pl.when(middle)
                def _():
                    landed(q, other)
                    landed(q, far)
                    _, lo, n, i = todo[q]
                    base = peers[i] * rows + lo

                    def square_sum(t, acc):
                        v = x[pl.ds(pl.multiple_of(base + t * 16, 16), 16), :].astype(F32)
                        return acc + v * v

                    part = lax.fori_loop(0, n // 16, square_sum, jnp.zeros(ssq.shape, F32))
                    ssq[...] = part if q == 0 else ssq[...] + part

        def drain():
            for q in range(len(todo)):
                copy_own(q).wait_send()

                @pl.when(middle)
                def _():
                    copy_on(q).wait_send()

        return stage, finish, drain

    gathers = [gather(0), gather(1)]

    def on_core(core, fn):
        @pl.when(c == core)
        def _():
            fn()

    size, width = x.shape
    block = 256
    nblk = size // block

    def column(s):
        return pl.ds(pl.multiple_of(s * cols, cols), cols)

    def row_block(r):
        return pl.ds(pl.multiple_of(r * rows, rows), rows)

    def normalize():
        inv = 1.0 / (jnp.sqrt(jnp.sum(ssq[...], keepdims=True)) + NORM_EPS)

        @pl.loop(0, size // 16)
        def _(i):
            sl = pl.ds(pl.multiple_of(i * 16, 16), 16)
            x[sl, :] = (x[sl, :].astype(F32) * inv).astype(BF16)

    def square():
        for i in range(nblk):
            for j in range(i, nblk):
                blk = lax.dot_general(x[i * block:(i + 1) * block, :], x[j * block:(j + 1) * block, :], NT,
                                      preferred_element_type=F32).astype(BF16)
                gram[i * block:(i + 1) * block, j * block:(j + 1) * block] = blk
                if j > i:
                    gram[j * block:(j + 1) * block, i * block:(i + 1) * block] = blk.T

    def polynomial():
        for i in range(nblk):
            ra, rb = i * block, (i + 1) * block
            strip = (COEF_B * gram[ra:rb, ra:].astype(F32) + COEF_C * dot(gram[ra:rb, :], gram[:, ra:])).astype(BF16)
            poly[ra:rb, ra:] = strip
            for j in range(i + 1, nblk):
                poly[j * block:(j + 1) * block, ra:rb] = strip[:, j * block - ra:(j + 1) * block - ra].T

    def update(lo, hi):
        @pl.loop(lo, hi)
        def _(t):
            cs = column(t)
            xc = x[:, cs]
            x[:, cs] = (COEF_A * xc.astype(F32) + dot(poly[...], xc)).astype(BF16)

    def in_middle(fn):
        @pl.when(middle)
        def _():
            fn()

    def whole(core):
        gathers[core][1]()
        gathers[core][2]()
        in_middle(normalize)

    def poly_and_update():
        polynomial()
        update(0, 1)

    head = {
        HEAD: lambda: whole(0),
        HEAD + 1: lambda: in_middle(square),
        HEAD + 2: lambda: in_middle(poly_and_update),
        HEAD + 3: lambda: in_middle(lambda: update(1, 2)),
        HEAD + 4: lambda: in_middle(lambda: update(2, 3)),
        HEAD + 5: lambda: in_middle(lambda: update(3, TP)),
    }

    chip_sum(0)
    chip_sum(1)
    copy_y(0).start()
    copy_y(1).start()
    sent = 2
    for k in range(npiece):
        for j in range(sent, SENT[k]):
            chip_sum(j)
        update_piece(k)
        for j in range(sent, SENT[k]):
            copy_y(j).start()
        sent = SENT[k]
        for (core, chip), todo in STAGES.items():
            if k in todo:
                @pl.when(jnp.logical_and(c == core, y == chip))
                def _():
                    for t in todo[k]:
                        gathers[core][0](t)
        if k in head:
            on_core(0, head[k])

    def copy_w(i):
        return mesh_copy(weight.at[peers[i]], wg.at[i - 1], pw.at[i], rw.at[i], dp=peers[i])

    wv = own_me
    load_w = [pltpu.make_async_copy(weight.at[peers[i]], wv.at[i], lw.at[i]) for i in range(DP)]
    for i in range(1, DP):
        copy_w(i).start()
    for cp in load_w:
        cp.start()

    on_core(1, lambda: whole(1))

    @pl.when(middle)
    def _():
        def step(i, carry):
            square()
            polynomial()

            @pl.when(i < NS_STEPS - 1)
            def _():
                update(0, TP)
            return carry
        lax.fori_loop(1 - c, NS_STEPS, step, 0)

    hrows = rows // 2

    def half_block(r, h):
        return pl.ds(pl.multiple_of(r * rows + h * hrows, hrows), hrows)

    def half(h):
        return pl.ds(h * hrows, hrows)

    def copy_e(i, h):
        blk = half_block(peers[i], h)
        return mesh_copy(x5e.at[blk, :], x5.at[blk, :], se.at[i, h], re.at[i, h], tp=end)

    def last(i, s, dst):
        blk = row_block(peers[i])
        dst[blk, :] = (COEF_A * x[blk, column(s)].astype(F32) + dot(poly[blk, :], x[:, column(s)])).astype(BF16)

    def apply(w, v, mat):
        return w - lr[mat] * (out_scale * v.astype(F32) + decay[0] * w)

    def each(h, fn):
        @pl.loop(0, hrows // STEP)
        def _(i):
            fn(pl.multiple_of(h * hrows + i * STEP, STEP))

    def to_partner(src, mat, r, h, sem):
        return mesh_copy(src, wb.at[mat, half_block(r, h), :], sem, rd.at[mat, r, h], dp=partner)

    def send_x(i, h):
        return mesh_copy(x5.at[half_block(peers[i], h), :], xr.at[me, half(h), :], sx.at[i, h], rx.at[me, h], dp=peers[i])

    def send_w(i, h):
        return mesh_copy(ws.at[i, half(h), :], wb.at[me, half_block(peers[i], h), :], sw.at[i, h], rwb.at[me, h], dp=peers[2 + i])

    def share_own(i, h):
        return to_partner(ws.at[i, half(h), :], me, peers[i], h, sd.at[i, h])

    def share_mine(i, h):
        return to_partner(wo.at[i, half(h), :], peers[i], me, h, sm2.at[i, h])

    def pass_on(i, h):
        return to_partner(wb.at[peers[i], half_block(yp, h), :], peers[i], yp, h, sf.at[i, h])

    def store_b(i, h):
        return pltpu.make_async_copy(ws.at[i, half(h), :], wb.at[me, half_block(peers[i], h), :], sl_b.at[i, h])

    def store_o(i, h):
        return pltpu.make_async_copy(wo.at[i, half(h), :], wb.at[peers[i], half_block(me, h), :], sl_o.at[i, h])

    def store_n(i, h):
        return pltpu.make_async_copy(wv.at[i, half(h), :], w_new.at[peers[i], half(h), :], sl_n.at[i, h])

    halves = (0, 1)

    for i in (2, 3, 0, 1):
        r = peers[i]

        @pl.when(middle)
        def _():
            last(i, end, x5e)
            for h in halves:
                copy_e(i, h).start()
            last(i, z, x5)

        if i == 0:
            load_w[0].wait()
        else:
            copy_w(i).wait_recv()
        for h in halves:
            @pl.when(jnp.logical_not(middle))
            def _():
                copy_e(i, h).wait_recv()

            if i > 0:
                send_x(i, h).start()

            def rows_of(lo, i=i, r=r):
                sl = pl.ds(lo, STEP)
                v = x5[pl.ds(pl.multiple_of(r * rows + lo, STEP), STEP), :]
                if i == 0:
                    w = apply(wv[0, sl, :], v, me)
                    wv[0, sl, :] = w
                else:
                    w = apply(wg[i - 1, sl, :], v, me)
                ws[i, sl, :] = w.astype(BF16)
            each(h, rows_of)
            if i < 2:
                send_w(i, h).start()
            if i != 1:
                share_own(i, h).start()
            store_b(i, h).start()
            if i == 0:
                store_n(0, h).start()

    def mine(i):
        mat = peers[i]
        load_w[i].wait()
        for h in halves:
            mesh_copy(x5.at[half_block(me, h), :], xr.at[mat, half(h), :], sx.at[0, h], rx.at[mat, h], dp=mat).wait_recv()

            def rows_of(lo):
                sl = pl.ds(lo, STEP)
                w = apply(wv[i, sl, :], xr[mat, sl, :], mat)
                wv[i, sl, :] = w
                wo[i, sl, :] = w.astype(BF16)
            each(h, rows_of)
            if i > 1:
                share_mine(i, h).start()
            store_n(i, h).start()
            store_o(i, h).start()

    def relay(i):
        for h in halves:
            mesh_copy(ws.at[0, half(h), :], wb.at[peers[i], half_block(yp, h), :], sw.at[0, h], rwb.at[peers[i], h],
                      dp=peers[i]).wait_recv()
            pass_on(i, h).start()

    def core0_order():
        mine(2)
        relay(2)
        mine(1)
        mine(3)
        relay(3)

    def core1_order():
        mine(1)
        mine(3)
        relay(3)
        mine(2)
        relay(2)

    for k in range(npiece):
        copy_a(k).wait_send()
        copy_b(k).wait_send()
        copy_y(k).wait_send()
        store_mom(k).wait()

        @pl.when(me != ORDER[k][0])
        def _():
            copy_u(k).wait_send()
    for i in range(1, DP):
        copy_w(i).wait_send()

    on_core(0, core0_order)
    on_core(1, core1_order)

    for mat, r in ((partner, partner), (partner, yp), (partner, diag), (yp, partner), (diag, partner), (yp, diag), (diag, diag)):
        for h in halves:
            to_partner(ws.at[0, half(h), :], mat, r, h, sd.at[0, h]).wait_recv()

    for i in range(DP):
        for h in halves:
            @pl.when(middle)
            def _():
                copy_e(i, h).wait_send()

            if i > 0:
                send_x(i, h).wait_send()
                store_o(i, h).wait()
            if i < 2:
                send_w(i, h).wait_send()
            if i != 1:
                share_own(i, h).wait_send()
            if i > 1:
                share_mine(i, h).wait_send()
                pass_on(i, h).wait_send()
            store_b(i, h).wait()
            store_n(i, h).wait()


def muon(grad, mom, weight, lr, decay, out_scale):
    _, mats, all_rows, cols = grad.shape
    rows = mom.shape[1]
    n = len(ORDER)
    nq = DP * MAX_PARTS
    dma = pltpu.SemaphoreType.DMA
    hbm = pl.BlockSpec(memory_space=pl.ANY)
    smem = pl.BlockSpec(memory_space=pltpu.SMEM)
    f32 = pltpu.VMEM((mats, rows, cols), F32)
    b16 = pltpu.VMEM((mats, rows, cols), BF16)
    square = pltpu.VMEM((all_rows, all_rows), BF16)
    slab = pltpu.VMEM((all_rows, cols), BF16)
    return pl.pallas_call(
        functools.partial(muon_kernel, out_scale),
        out_shape=(jax.ShapeDtypeStruct(mom.shape, F32), jax.ShapeDtypeStruct(weight.shape, F32),
                   jax.ShapeDtypeStruct((mats, all_rows, cols), BF16)),
        in_specs=[hbm] * 3 + [smem] * 2,
        out_specs=[hbm] * 3,
        scratch_shapes=[f32] * 6 + [b16, pltpu.VMEM((all_rows, TP * cols), BF16), square, square, slab, slab,
                                    pltpu.VMEM((DP - 1, rows, cols), F32), b16, b16, b16, pltpu.VMEM((16, TP * cols), F32)]
        + [dma((n,))] * 11 + [dma((DP, MAX_PARTS)), dma((nq,)), dma((nq,)), dma((TP, nq))]
        + [dma((DP,))] * 3 + [dma((DP, 2))] * 12 + [dma((DP, DP, 2))],
        compiler_params=pltpu.CompilerParams(collective_id=0, has_side_effects=True, vmem_limit_bytes=67043328),
        name="muon",
    )(grad, mom, weight, lr, decay)


def copy_kernel(*refs):
    n = len(refs) // 4
    sources, outs, bufs, sems = refs[:n], refs[n:2 * n], refs[2 * n:3 * n], refs[3 * n:]
    reads, writes = [], []
    for src, out, buf, sem in zip(sources, outs, bufs, sems):
        for i in range(src.shape[0]):
            reads.append(pltpu.make_async_copy(src.at[i], buf.at[i], sem.at[0, i]))
            writes.append(pltpu.make_async_copy(buf.at[i], out.at[i], sem.at[1, i]))
    for cp in reads:
        cp.start()
    for rd, wr in zip(reads, writes):
        rd.wait()
        wr.start()
    for cp in writes:
        cp.wait()


def results(*arrays):
    flat = [v.reshape(-1, 256, v.shape[-1]) for v in arrays]
    hbm = pl.BlockSpec(memory_space=pl.ANY)
    out = pl.pallas_call(
        copy_kernel,
        out_shape=tuple(jax.ShapeDtypeStruct(v.shape, v.dtype) for v in flat),
        in_specs=[hbm] * len(flat),
        out_specs=(hbm,) * len(flat),
        scratch_shapes=[pltpu.VMEM(v.shape, v.dtype) for v in flat]
        + [pltpu.SemaphoreType.DMA((2, v.shape[0])) for v in flat],
        compiler_params=pltpu.CompilerParams(vmem_limit_bytes=67043328),
        name="results",
    )(*flat)
    return tuple(o.reshape(v.shape) for o, v in zip(out, arrays))


def solution(mesh):
    def local_step(grad, mom, weight, learn_rate, decay_rate):
        out_scale = 0.2 * math.sqrt(max(grad.shape[2], grad.shape[3] * TP))
        return results(*muon(grad, mom, weight, learn_rate, decay_rate.reshape(1), out_scale))

    return jax.shard_map(
        local_step,
        mesh=mesh,
        in_specs=(P(("rep", "dp"), None, None, "tp"), P("rep", "dp", "tp"), P("rep", "dp", "tp"), P("rep"), P()),
        out_specs=(P("rep", "dp", "tp"), P("rep", "dp", "tp"), P("rep", None, "tp")),
        check_vma=False,
    )
```

```python
import functools
import math

import jax
import jax.numpy as jnp
from jax import lax
from jax.experimental import pallas as pl
from jax.experimental.pallas import tpu as pltpu
from jax.sharding import PartitionSpec as P

MOMENTUM = 0.95
NS_STEPS = 5
COEF_A = 3.4445
COEF_B = -4.7750
COEF_C = 2.0315
NORM_EPS = 1e-7

DP = 4
TP = 4
F32 = jnp.float32
BF16 = jnp.bfloat16
NT = (((1,), (1,)), ((), ()))

ORDER = [(m, p) for p in range(4) for m in (0, 2)] + [(m, p) for p in range(5) for m in (1, 3)]
PARTS = {0: [(0, 16), (16, 16), (32, 16), (48, 16)], 1: [(0, 16), (16, 16), (32, 16), (48, 8), (56, 8)]}
MAX_PARTS = 5
NPIECE = len(ORDER)
SENT = [k + 3 if k < 14 else NPIECE for k in range(NPIECE)]


def stages(core, chip):
    first, parts = (0, 4) if core == 0 else (8, 5)
    out = {}
    for p in range(parts):
        k = first + 2 * p + chip
        out.setdefault(k, []).extend((4 * p, 4 * p + 1))
        out.setdefault(min(k + 1, NPIECE - 1), []).extend((4 * p + 2, 4 * p + 3))
    out.setdefault(min(k + 2, NPIECE - 1), []).append(4 * parts)
    return out


STAGES = {(core, chip): stages(core, chip) for core in range(2) for chip in range(2)}
HEAD = 9
STEP = 32


def mesh_copy(src, dst, send, recv, **axes):
    return pltpu.make_async_remote_copy(
        src_ref=src, dst_ref=dst, send_sem=send, recv_sem=recv,
        device_id=axes, device_id_type=pl.DeviceIdType.MESH)


def dot(a, b):
    return jnp.dot(a, b, preferred_element_type=F32)


def muon_kernel(out_scale, grad, mom, weight, lr, decay,
                mom_new, w_new, wb,
                own_yp, own_me, recv_a, recv_b, recv_y, momb, ub, x, gram, poly, x5, x5e, wg, xr, ws, wo, ssq,
                ld_yp, ld_me, ld_mom, sa, ra, sb, rb, sy, ry, su, sm, ru,
                zs, zf, zr, pw, rw, lw, se, re, sx, rx, sw, rwb, sd, sm2, sf, sl_b, sl_o, sl_n, rd):
    me = lax.axis_index("dp")
    z = lax.axis_index("tp")
    y, c = lax.div(me, 2), lax.rem(me, 2)
    partner, yp, diag = 2 * y + (1 - c), 2 * (1 - y) + c, 2 * (1 - y) + (1 - c)
    peers = (me, partner, yp, diag)
    rows, cols = mom.shape[1], mom.shape[2]
    unit = rows // 64
    npiece = len(ORDER)
    middle = jnp.logical_and(z > 0, z < TP - 1)
    left = z < TP // 2
    nb = jnp.where(left, z + 1, z - 1)
    other = TP - 1 - z
    end = jnp.where(left, 0, TP - 1)
    far = TP - 1 - end

    barrier = pltpu.get_barrier_semaphore()
    for peer in peers[1:]:
        pl.semaphore_signal(barrier, inc=1, device_id={"dp": peer}, device_id_type=pl.DeviceIdType.MESH)

    @pl.when(z > 0)
    def _():
        pl.semaphore_signal(barrier, inc=1, device_id={"tp": z - 1}, device_id_type=pl.DeviceIdType.MESH)

    @pl.when(z < TP - 1)
    def _():
        pl.semaphore_signal(barrier, inc=1, device_id={"tp": z + 1}, device_id_type=pl.DeviceIdType.MESH)

    def span(k):
        m, p = ORDER[k]
        lo, n = PARTS[m % 2][p]
        return m, p, lo * unit, n * unit

    def grad_rows(r, k):
        m, _, lo, n = span(k)
        return grad.at[0, m, pl.ds(pl.multiple_of(r * rows + lo, 16), n), :]

    def piece(buf, k):
        m, _, lo, n = span(k)
        return buf.at[m, pl.ds(lo, n), :]

    def load_yp(k):
        return pltpu.make_async_copy(grad_rows(yp, k), piece(own_yp, k), ld_yp)

    def load_me(k):
        return pltpu.make_async_copy(grad_rows(me, k), piece(own_me, k), ld_me)

    def load_mom(k):
        return pltpu.make_async_copy(piece(mom, k), piece(momb, k), ld_mom)

    def copy_a(k):
        return mesh_copy(grad_rows(diag, k), piece(recv_a, k), sa, ra.at[k], dp=partner)

    def copy_b(k):
        return mesh_copy(grad_rows(partner, k), piece(recv_b, k), sb, rb, dp=partner)

    def copy_y(k):
        return mesh_copy(piece(own_yp, k), piece(recv_y, k), sy, ry.at[k], dp=yp)

    def store_mom(k):
        return pltpu.make_async_copy(piece(momb, k), piece(mom_new, k), sm)

    def x_block(r, lo, n, s):
        return x.at[pl.ds(pl.multiple_of(r * rows + lo, 16), n), pl.ds(pl.multiple_of(s * cols, cols), cols)]

    def copy_u(k):
        m, p, lo, n = span(k)
        return mesh_copy(piece(ub, k), x_block(me, lo, n, z), su, ru.at[me, p], dp=m)

    for k in range(npiece):
        load_yp(k).start()
    for k in range(npiece):
        load_me(k).start()
        load_mom(k).start()
    pl.semaphore_wait(barrier, 3 + jnp.where(z > 0, 1, 0) + jnp.where(z < TP - 1, 1, 0))
    for k in range(npiece):
        copy_a(k).start()
    for k in range(npiece):
        copy_b(k).start()

    def chip_sum(k):
        m, _, lo, n = span(k)
        if k == 0:
            pltpu.make_async_copy(own_yp, own_yp, ld_yp).wait()
        copy_a(k).wait_recv()

        @pl.loop(0, n // STEP)
        def _(i):
            sl = pl.ds(pl.multiple_of(lo + i * STEP, STEP), STEP)
            own_yp[m, sl, :] = own_yp[m, sl, :] + recv_a[m, sl, :]

    def update_piece(k):
        m, _, lo, n = span(k)
        if k == 0:
            pltpu.make_async_copy(own_me, own_me, ld_me).wait()
            pltpu.make_async_copy(momb, momb, ld_mom).wait()
            mesh_copy(recv_b, recv_b, sb, rb, dp=partner).wait_recv()
        copy_y(k).wait_recv()

        @pl.loop(0, n // STEP)
        def _(i):
            sl = pl.ds(pl.multiple_of(lo + i * STEP, STEP), STEP)
            g = (own_me[m, sl, :] + recv_b[m, sl, :] + recv_y[m, sl, :]) * (1.0 / DP)
            mn = MOMENTUM * momb[m, sl, :] + g
            momb[m, sl, :] = mn
            ub[m, sl, :] = (g + MOMENTUM * mn).astype(BF16)

        @pl.when(me == m)
        def _():
            x[pl.ds(pl.multiple_of(me * rows + lo, 16), n), pl.ds(pl.multiple_of(z * cols, cols), cols)] = ub[m, lo:lo + n, :]

        @pl.when(me != m)
        def _():
            copy_u(k).start()

        store_mom(k).start()

    def gather(core):
        todo = [(p, lo * unit, n * unit, i) for p, (lo, n) in enumerate(PARTS[core]) for i in range(DP)]

        def copy_own(q):
            _, lo, n, i = todo[q]
            blk = x_block(peers[i], lo, n, z)
            return mesh_copy(blk, blk, zs, zr.at[jnp.where(middle, 1, 0), q], tp=nb)

        def copy_on(q):
            _, lo, n, i = todo[q]
            blk = x_block(peers[i], lo, n, end)
            return mesh_copy(blk, blk, zf, zr.at[2, q], tp=other)

        def landed(q, s, kind):
            _, lo, n, i = todo[q]
            blk = x_block(peers[i], lo, n, s)
            mesh_copy(blk, blk, zs, zr.at[kind, q], tp=nb).wait_recv()

        def stage(t):
            if t < len(todo):
                p, lo, n, i = todo[t]
                if i > 0:
                    mesh_copy(ub.at[0, pl.ds(0, n), :], x_block(peers[i], lo, n, z), su, ru.at[peers[i], p],
                              dp=peers[i]).wait_recv()
                copy_own(t).start()
            if t > 0:
                @pl.when(middle)
                def _():
                    landed(t - 1, end, 0)
                    copy_on(t - 1).start()

        def finish():
            for q in range(len(todo)):
                @pl.when(middle)
                def _():
                    landed(q, other, 1)
                    landed(q, far, 2)
                    _, lo, n, i = todo[q]
                    base = peers[i] * rows + lo

                    def square_sum(t, acc):
                        v = x[pl.ds(pl.multiple_of(base + t * 16, 16), 16), :].astype(F32)
                        return acc + v * v

                    part = lax.fori_loop(0, n // 16, square_sum, jnp.zeros(ssq.shape, F32))
                    ssq[...] = part if q == 0 else ssq[...] + part

        def drain():
            slab = x.at[:, pl.ds(0, cols)]
            mesh_copy(slab, slab, zs, zr.at[0, 0], tp=nb).wait_send()

            @pl.when(middle)
            def _():
                mesh_copy(slab, slab, zf, zr.at[0, 0], tp=other).wait_send()

        return stage, finish, drain

    gathers = [gather(0), gather(1)]

    def on_core(core, fn):
        @pl.when(c == core)
        def _():
            fn()

    size, width = x.shape
    block = 256
    nblk = size // block

    def column(s):
        return pl.ds(pl.multiple_of(s * cols, cols), cols)

    def row_block(r):
        return pl.ds(pl.multiple_of(r * rows, rows), rows)

    def normalize():
        inv = 1.0 / (jnp.sqrt(jnp.sum(ssq[...], keepdims=True)) + NORM_EPS)

        @pl.loop(0, size // 16)
        def _(i):
            sl = pl.ds(pl.multiple_of(i * 16, 16), 16)
            x[sl, :] = (x[sl, :].astype(F32) * inv).astype(BF16)

    def square():
        for i in range(nblk):
            for j in range(i, nblk):
                blk = lax.dot_general(x[i * block:(i + 1) * block, :], x[j * block:(j + 1) * block, :], NT,
                                      preferred_element_type=F32).astype(BF16)
                gram[i * block:(i + 1) * block, j * block:(j + 1) * block] = blk
                if j > i:
                    gram[j * block:(j + 1) * block, i * block:(i + 1) * block] = blk.T

    def polynomial():
        for i in range(nblk):
            ra, rb = i * block, (i + 1) * block
            strip = (COEF_B * gram[ra:rb, ra:].astype(F32) + COEF_C * dot(gram[ra:rb, :], gram[:, ra:])).astype(BF16)
            poly[ra:rb, ra:] = strip
            for j in range(i + 1, nblk):
                poly[j * block:(j + 1) * block, ra:rb] = strip[:, j * block - ra:(j + 1) * block - ra].T

    def update(lo, hi):
        @pl.loop(lo, hi)
        def _(t):
            cs = column(t)
            xc = x[:, cs]
            x[:, cs] = (COEF_A * xc.astype(F32) + dot(poly[...], xc)).astype(BF16)

    def in_middle(fn):
        @pl.when(middle)
        def _():
            fn()

    def whole(core):
        gathers[core][1]()
        gathers[core][2]()
        in_middle(normalize)

    def poly_and_update():
        polynomial()
        update(0, 1)

    head = {
        HEAD: lambda: whole(0),
        HEAD + 1: lambda: in_middle(square),
        HEAD + 2: lambda: in_middle(poly_and_update),
        HEAD + 3: lambda: in_middle(lambda: update(1, 2)),
        HEAD + 4: lambda: in_middle(lambda: update(2, 3)),
        HEAD + 5: lambda: in_middle(lambda: update(3, TP)),
    }

    chip_sum(0)
    chip_sum(1)
    copy_y(0).start()
    copy_y(1).start()
    sent = 2
    for k in range(npiece):
        for j in range(sent, SENT[k]):
            chip_sum(j)
        update_piece(k)
        for j in range(sent, SENT[k]):
            copy_y(j).start()
        sent = SENT[k]
        for (core, chip), todo in STAGES.items():
            if k in todo:
                @pl.when(jnp.logical_and(c == core, y == chip))
                def _():
                    for t in todo[k]:
                        gathers[core][0](t)
        if k in head:
            on_core(0, head[k])

    def copy_w(i):
        return mesh_copy(weight.at[peers[i]], wg.at[i - 1], pw, rw.at[i], dp=peers[i])

    wv = own_me
    load_w = [pltpu.make_async_copy(weight.at[peers[i]], wv.at[i], lw.at[i]) for i in range(DP)]
    for i in range(1, DP):
        copy_w(i).start()
    for cp in load_w:
        cp.start()

    on_core(1, lambda: whole(1))

    @pl.when(middle)
    def _():
        def step(i, carry):
            square()
            polynomial()

            @pl.when(i < NS_STEPS - 1)
            def _():
                update(0, TP)
            return carry
        lax.fori_loop(1 - c, NS_STEPS, step, 0)

    hrows = rows // 2

    def half_block(r, h):
        return pl.ds(pl.multiple_of(r * rows + h * hrows, hrows), hrows)

    def half(h):
        return pl.ds(h * hrows, hrows)

    def copy_e(i, h):
        blk = half_block(peers[i], h)
        return mesh_copy(x5e.at[blk, :], x5.at[blk, :], se, re.at[i, h], tp=end)

    def last(i, s, dst):
        blk = row_block(peers[i])
        dst[blk, :] = (COEF_A * x[blk, column(s)].astype(F32) + dot(poly[blk, :], x[:, column(s)])).astype(BF16)

    def apply(w, v, mat):
        return w - lr[mat] * (out_scale * v.astype(F32) + decay[0] * w)

    def each(h, fn):
        @pl.loop(0, hrows // STEP)
        def _(i):
            fn(pl.multiple_of(h * hrows + i * STEP, STEP))

    def to_partner(src, mat, r, h, sem, slot):
        return mesh_copy(src, wb.at[mat, half_block(r, h), :], sem, rd.at[slot, h], dp=partner)

    def send_x(i, h):
        return mesh_copy(x5.at[half_block(peers[i], h), :], xr.at[me, half(h), :], sx, rx.at[me, h], dp=peers[i])

    def send_w(i, h):
        return mesh_copy(ws.at[i, half(h), :], wb.at[me, half_block(peers[i], h), :], sw, rwb.at[me, h], dp=peers[2 + i])

    def share_own(i, h):
        return to_partner(ws.at[i, half(h), :], me, peers[i], h, sd, (0, None, 1, 2)[i])

    def share_mine(i, h):
        return to_partner(wo.at[i, half(h), :], peers[i], me, h, sm2, 1 + i)

    def pass_on(i, h):
        return to_partner(wb.at[peers[i], half_block(yp, h), :], peers[i], yp, h, sf, 3 + i)

    def store_b(i, h):
        return pltpu.make_async_copy(ws.at[i, half(h), :], wb.at[me, half_block(peers[i], h), :], sl_b)

    def store_o(i, h):
        return pltpu.make_async_copy(wo.at[i, half(h), :], wb.at[peers[i], half_block(me, h), :], sl_o)

    def store_n(i, h):
        return pltpu.make_async_copy(wv.at[i, half(h), :], w_new.at[peers[i], half(h), :], sl_n)

    halves = (0, 1)

    for i in (2, 3, 0, 1):
        r = peers[i]

        @pl.when(middle)
        def _():
            last(i, end, x5e)
            for h in halves:
                copy_e(i, h).start()
            last(i, z, x5)

        if i == 0:
            load_w[0].wait()
        else:
            copy_w(i).wait_recv()
        for h in halves:
            @pl.when(jnp.logical_not(middle))
            def _():
                copy_e(i, h).wait_recv()

            if i > 0:
                send_x(i, h).start()

            def rows_of(lo, i=i, r=r):
                sl = pl.ds(lo, STEP)
                v = x5[pl.ds(pl.multiple_of(r * rows + lo, STEP), STEP), :]
                if i == 0:
                    w = apply(wv[0, sl, :], v, me)
                    wv[0, sl, :] = w
                else:
                    w = apply(wg[i - 1, sl, :], v, me)
                ws[i, sl, :] = w.astype(BF16)
            each(h, rows_of)
            if i < 2:
                send_w(i, h).start()
            if i != 1:
                share_own(i, h).start()
            store_b(i, h).start()
            if i == 0:
                store_n(0, h).start()

    def mine(i):
        mat = peers[i]
        load_w[i].wait()
        for h in halves:
            mesh_copy(x5.at[half_block(me, h), :], xr.at[mat, half(h), :], sx, rx.at[mat, h], dp=mat).wait_recv()

            def rows_of(lo):
                sl = pl.ds(lo, STEP)
                w = apply(wv[i, sl, :], xr[mat, sl, :], mat)
                wv[i, sl, :] = w
                wo[i, sl, :] = w.astype(BF16)
            each(h, rows_of)
            if i > 1:
                share_mine(i, h).start()
            store_n(i, h).start()
            store_o(i, h).start()

    def relay(i):
        for h in halves:
            mesh_copy(ws.at[0, half(h), :], wb.at[peers[i], half_block(yp, h), :], sw, rwb.at[peers[i], h],
                      dp=peers[i]).wait_recv()
            pass_on(i, h).start()

    def core0_order():
        mine(2)
        relay(2)
        mine(1)
        mine(3)
        relay(3)

    def core1_order():
        mine(1)
        mine(3)
        relay(3)
        mine(2)
        relay(2)

    mesh_copy(recv_a, recv_a, sa, ra.at[0], dp=partner).wait_send()
    mesh_copy(recv_b, recv_b, sb, rb, dp=partner).wait_send()
    mesh_copy(own_yp, own_yp, sy, ry.at[0], dp=yp).wait_send()
    pltpu.make_async_copy(momb, momb, sm).wait()
    mesh_copy(ub.at[1:DP], ub.at[1:DP], su, ru.at[0, 0], dp=partner).wait_send()
    mesh_copy(wg, wg, pw, rw.at[0], dp=partner).wait_send()

    on_core(0, core0_order)
    on_core(1, core1_order)

    arrivals = ((partner, partner), (partner, diag), (partner, yp), (diag, partner), (yp, partner), (diag, diag), (yp, diag))
    for slot, (mat, r) in enumerate(arrivals):
        for h in halves:
            to_partner(ws.at[0, half(h), :], mat, r, h, sd, slot).wait_recv()

    @pl.when(middle)
    def _():
        mesh_copy(x5e, x5e, se, re.at[0, 0], tp=end).wait_send()

    def sent(n, sem, slot):
        mesh_copy(ws.at[0:n], ws.at[0:n], sem, slot, dp=partner).wait_send()

    sent(3, sx, rx.at[0, 0])
    sent(2, sw, rwb.at[0, 0])
    sent(3, sd, rd.at[0, 0])
    sent(2, sm2, rd.at[0, 0])
    sent(2, sf, rd.at[0, 0])
    pltpu.make_async_copy(ws, ws, sl_b).wait()
    pltpu.make_async_copy(wo.at[1:DP], wo.at[1:DP], sl_o).wait()
    pltpu.make_async_copy(wv, wv, sl_n).wait()


def muon(grad, mom, weight, lr, decay, out_scale):
    _, mats, all_rows, cols = grad.shape
    rows = mom.shape[1]
    n = len(ORDER)
    nq = DP * MAX_PARTS
    dma = pltpu.SemaphoreType.DMA
    hbm = pl.BlockSpec(memory_space=pl.ANY)
    smem = pl.BlockSpec(memory_space=pltpu.SMEM)
    f32 = pltpu.VMEM((mats, rows, cols), F32)
    b16 = pltpu.VMEM((mats, rows, cols), BF16)
    square = pltpu.VMEM((all_rows, all_rows), BF16)
    slab = pltpu.VMEM((all_rows, cols), BF16)
    return pl.pallas_call(
        functools.partial(muon_kernel, out_scale),
        out_shape=(jax.ShapeDtypeStruct(mom.shape, F32), jax.ShapeDtypeStruct(weight.shape, F32),
                   jax.ShapeDtypeStruct((mats, all_rows, cols), BF16)),
        in_specs=[hbm] * 3 + [smem] * 2,
        out_specs=[hbm] * 3,
        scratch_shapes=[f32] * 6 + [b16, pltpu.VMEM((all_rows, TP * cols), BF16), square, square, slab, slab,
                                    pltpu.VMEM((DP - 1, rows, cols), F32), b16, b16, b16, pltpu.VMEM((16, TP * cols), F32)]
        + [dma] * 4 + [dma((n,)), dma, dma, dma, dma((n,)), dma, dma, dma((DP, MAX_PARTS)), dma, dma, dma((3, nq)), dma, dma((DP,)),
           dma((DP,)), dma, dma((DP, 2)), dma, dma((DP, 2)), dma, dma((DP, 2))] + [dma] * 6 + [dma((7, 2))],
        compiler_params=pltpu.CompilerParams(collective_id=0, has_side_effects=True, vmem_limit_bytes=67043328),
        name="muon",
    )(grad, mom, weight, lr, decay)


def copy_kernel(*refs):
    n = len(refs) // 4
    sources, outs, bufs, sems = refs[:n], refs[n:2 * n], refs[2 * n:3 * n], refs[3 * n:]
    reads, writes = [], []
    for src, out, buf, sem in zip(sources, outs, bufs, sems):
        for i in range(src.shape[0]):
            reads.append(pltpu.make_async_copy(src.at[i], buf.at[i], sem.at[0, i]))
            writes.append(pltpu.make_async_copy(buf.at[i], out.at[i], sem.at[1, i]))
    for cp in reads:
        cp.start()
    for rd, wr in zip(reads, writes):
        rd.wait()
        wr.start()
    for cp in writes:
        cp.wait()


def results(*arrays):
    flat = [v.reshape(-1, 256, v.shape[-1]) for v in arrays]
    hbm = pl.BlockSpec(memory_space=pl.ANY)
    out = pl.pallas_call(
        copy_kernel,
        out_shape=tuple(jax.ShapeDtypeStruct(v.shape, v.dtype) for v in flat),
        in_specs=[hbm] * len(flat),
        out_specs=(hbm,) * len(flat),
        scratch_shapes=[pltpu.VMEM(v.shape, v.dtype) for v in flat]
        + [pltpu.SemaphoreType.DMA((2, v.shape[0])) for v in flat],
        compiler_params=pltpu.CompilerParams(vmem_limit_bytes=67043328),
        name="results",
    )(*flat)
    return tuple(o.reshape(v.shape) for o, v in zip(out, arrays))


def solution(mesh):
    def local_step(grad, mom, weight, learn_rate, decay_rate):
        out_scale = 0.2 * math.sqrt(max(grad.shape[2], grad.shape[3] * TP))
        return results(*muon(grad, mom, weight, learn_rate, decay_rate.reshape(1), out_scale))

    return jax.shard_map(
        local_step,
        mesh=mesh,
        in_specs=(P(("rep", "dp"), None, None, "tp"), P("rep", "dp", "tp"), P("rep", "dp", "tp"), P("rep"), P()),
        out_specs=(P("rep", "dp", "tp"), P("rep", "dp", "tp"), P("rep", None, "tp")),
        check_vma=False,
    )
```

```python
import functools
import math

import jax
import jax.numpy as jnp
from jax import lax
from jax.experimental import pallas as pl
from jax.experimental.pallas import tpu as pltpu
from jax.sharding import PartitionSpec as P

MOMENTUM = 0.95
NS_STEPS = 5
COEF_A = 3.4445
COEF_B = -4.7750
COEF_C = 2.0315
NORM_EPS = 1e-7

DP = 4
TP = 4
F32 = jnp.float32
BF16 = jnp.bfloat16
NT = (((1,), (1,)), ((), ()))

ORDER = [(m, p) for p in range(4) for m in (0, 2)] + [(m, p) for p in range(5) for m in (1, 3)]
PARTS = {0: [(0, 16), (16, 16), (32, 16), (48, 16)], 1: [(0, 16), (16, 16), (32, 16), (48, 8), (56, 8)]}
MAX_PARTS = 5
NPIECE = len(ORDER)
SENT = [k + 3 if k < 14 else NPIECE for k in range(NPIECE)]


def stages(core, chip):
    first, parts = (0, 4) if core == 0 else (8, 5)
    out = {}
    for p in range(parts):
        k = first + 2 * p + chip
        out.setdefault(k, []).extend((4 * p, 4 * p + 1))
        out.setdefault(min(k + 1, NPIECE - 1), []).extend((4 * p + 2, 4 * p + 3))
    out.setdefault(min(k + 2, NPIECE - 1), []).append(4 * parts)
    return out


STAGES = {(core, chip): stages(core, chip) for core in range(2) for chip in range(2)}
HEAD = 9
STEP = 32


def mesh_copy(src, dst, send, recv, **axes):
    return pltpu.make_async_remote_copy(
        src_ref=src, dst_ref=dst, send_sem=send, recv_sem=recv,
        device_id=axes, device_id_type=pl.DeviceIdType.MESH)


def dot(a, b):
    return jnp.dot(a, b, preferred_element_type=F32)


def muon_kernel(out_scale, grad, mom, weight, lr, decay,
                mom_new, w_new, wb,
                own_yp, own_me, recv_a, recv_b, recv_y, momb, ub, x, gram, poly, x5, x5e, wg, xr, ws, wo, ssq,
                ld_yp, ld_me, ld_mom, sa, ra, sb, rb, sy, ry, su, sm, ru,
                zs, zf, zr, pw, rw, lw, se, re, sx, rx, sw, rwb, sd, sm2, sf, sl_b, sl_o, sl_n, rd):
    me = lax.axis_index("dp")
    z = lax.axis_index("tp")
    y, c = lax.div(me, 2), lax.rem(me, 2)
    partner, yp, diag = 2 * y + (1 - c), 2 * (1 - y) + c, 2 * (1 - y) + (1 - c)
    peers = (me, partner, yp, diag)
    rows, cols = mom.shape[1], mom.shape[2]
    unit = rows // 64
    npiece = len(ORDER)
    middle = jnp.logical_and(z > 0, z < TP - 1)
    left = z < TP // 2
    nb = jnp.where(left, z + 1, z - 1)
    other = TP - 1 - z
    end = jnp.where(left, 0, TP - 1)
    far = TP - 1 - end

    barrier = pltpu.get_barrier_semaphore()
    for peer in peers[1:]:
        pl.semaphore_signal(barrier, inc=1, device_id={"dp": peer}, device_id_type=pl.DeviceIdType.MESH)

    @pl.when(z > 0)
    def _():
        pl.semaphore_signal(barrier, inc=1, device_id={"tp": z - 1}, device_id_type=pl.DeviceIdType.MESH)

    @pl.when(z < TP - 1)
    def _():
        pl.semaphore_signal(barrier, inc=1, device_id={"tp": z + 1}, device_id_type=pl.DeviceIdType.MESH)

    def span(k):
        m, p = ORDER[k]
        lo, n = PARTS[m % 2][p]
        return m, p, lo * unit, n * unit

    def grad_rows(r, k):
        m, _, lo, n = span(k)
        return grad.at[0, m, pl.ds(pl.multiple_of(r * rows + lo, 16), n), :]

    def piece(buf, k):
        m, _, lo, n = span(k)
        return buf.at[m, pl.ds(lo, n), :]

    def load_yp(k):
        return pltpu.make_async_copy(grad_rows(yp, k), piece(own_yp, k), ld_yp.at[0 if k < 2 else 1])

    def load_me(k):
        return pltpu.make_async_copy(grad_rows(me, k), piece(own_me, k), ld_me)

    def load_mom(k):
        return pltpu.make_async_copy(piece(mom, k), piece(momb, k), ld_mom)

    def copy_a(k):
        return mesh_copy(grad_rows(diag, k), piece(recv_a, k), sa, ra.at[k], dp=partner)

    def copy_b(k):
        return mesh_copy(grad_rows(partner, k), piece(recv_b, k), sb, rb, dp=partner)

    def copy_y(k):
        return mesh_copy(piece(own_yp, k), piece(recv_y, k), sy, ry.at[k], dp=yp)

    def store_mom(k):
        return pltpu.make_async_copy(piece(momb, k), piece(mom_new, k), sm)

    def x_block(r, lo, n, s):
        return x.at[pl.ds(pl.multiple_of(r * rows + lo, 16), n), pl.ds(pl.multiple_of(s * cols, cols), cols)]

    def copy_u(k):
        m, p, lo, n = span(k)
        return mesh_copy(piece(ub, k), x_block(me, lo, n, z), su, ru.at[me, p], dp=m)

    for k in range(npiece):
        load_yp(k).start()
    pl.semaphore_wait(barrier, 3 + jnp.where(z > 0, 1, 0) + jnp.where(z < TP - 1, 1, 0))
    for k in range(npiece):
        copy_a(k).start()
    for k in range(npiece):
        copy_b(k).start()

    def chip_sum(k):
        m, _, lo, n = span(k)
        if k == 0:
            early = own_yp.at[0:2, 0:rows // 4]
            pltpu.make_async_copy(early, early, ld_yp.at[0]).wait()
        if k == 2:
            late = own_yp.at[:, 0:rows - rows // 8]
            pltpu.make_async_copy(late, late, ld_yp.at[1]).wait()
        copy_a(k).wait_recv()

        @pl.loop(0, n // STEP)
        def _(i):
            sl = pl.ds(pl.multiple_of(lo + i * STEP, STEP), STEP)
            own_yp[m, sl, :] = own_yp[m, sl, :] + recv_a[m, sl, :]

    def update_piece(k):
        m, _, lo, n = span(k)
        if k == 0:
            pltpu.make_async_copy(own_me, own_me, ld_me).wait()
            pltpu.make_async_copy(momb, momb, ld_mom).wait()
            mesh_copy(recv_b, recv_b, sb, rb, dp=partner).wait_recv()
        copy_y(k).wait_recv()

        @pl.loop(0, n // STEP)
        def _(i):
            sl = pl.ds(pl.multiple_of(lo + i * STEP, STEP), STEP)
            g = (own_me[m, sl, :] + recv_b[m, sl, :] + recv_y[m, sl, :]) * (1.0 / DP)
            mn = MOMENTUM * momb[m, sl, :] + g
            momb[m, sl, :] = mn
            ub[m, sl, :] = (g + MOMENTUM * mn).astype(BF16)

        @pl.when(me == m)
        def _():
            x[pl.ds(pl.multiple_of(me * rows + lo, 16), n), pl.ds(pl.multiple_of(z * cols, cols), cols)] = ub[m, lo:lo + n, :]

        @pl.when(me != m)
        def _():
            copy_u(k).start()

        store_mom(k).start()

    def gather(core):
        todo = [(p, lo * unit, n * unit, i) for p, (lo, n) in enumerate(PARTS[core]) for i in range(DP)]

        def copy_own(q):
            _, lo, n, i = todo[q]
            blk = x_block(peers[i], lo, n, z)
            return mesh_copy(blk, blk, zs, zr.at[jnp.where(middle, 1, 0), q], tp=nb)

        def copy_on(q):
            _, lo, n, i = todo[q]
            blk = x_block(peers[i], lo, n, end)
            return mesh_copy(blk, blk, zf, zr.at[2, q], tp=other)

        def landed(q, s, kind):
            _, lo, n, i = todo[q]
            blk = x_block(peers[i], lo, n, s)
            mesh_copy(blk, blk, zs, zr.at[kind, q], tp=nb).wait_recv()

        def stage(t):
            if t < len(todo):
                p, lo, n, i = todo[t]
                if i > 0:
                    mesh_copy(ub.at[0, pl.ds(0, n), :], x_block(peers[i], lo, n, z), su, ru.at[peers[i], p],
                              dp=peers[i]).wait_recv()
                copy_own(t).start()
            if t > 0:
                @pl.when(middle)
                def _():
                    landed(t - 1, end, 0)
                    copy_on(t - 1).start()

        def finish():
            for q in range(len(todo)):
                @pl.when(middle)
                def _():
                    landed(q, other, 1)
                    landed(q, far, 2)
                    _, lo, n, i = todo[q]
                    base = peers[i] * rows + lo

                    def square_sum(t, acc):
                        v = x[pl.ds(pl.multiple_of(base + t * 16, 16), 16), :].astype(F32)
                        return acc + v * v

                    part = lax.fori_loop(0, n // 16, square_sum, jnp.zeros(ssq.shape, F32))
                    ssq[...] = part if q == 0 else ssq[...] + part

        def drain():
            slab = x.at[:, pl.ds(0, cols)]
            mesh_copy(slab, slab, zs, zr.at[0, 0], tp=nb).wait_send()

            @pl.when(middle)
            def _():
                mesh_copy(slab, slab, zf, zr.at[0, 0], tp=other).wait_send()

        return stage, finish, drain

    gathers = [gather(0), gather(1)]

    def on_core(core, fn):
        @pl.when(c == core)
        def _():
            fn()

    size, width = x.shape
    block = 256
    nblk = size // block

    def column(s):
        return pl.ds(pl.multiple_of(s * cols, cols), cols)

    def row_block(r):
        return pl.ds(pl.multiple_of(r * rows, rows), rows)

    def normalize():
        inv = 1.0 / (jnp.sqrt(jnp.sum(ssq[...], keepdims=True)) + NORM_EPS)

        @pl.loop(0, size // 16)
        def _(i):
            sl = pl.ds(pl.multiple_of(i * 16, 16), 16)
            x[sl, :] = (x[sl, :].astype(F32) * inv).astype(BF16)

    def square():
        for i in range(nblk):
            for j in range(i, nblk):
                blk = lax.dot_general(x[i * block:(i + 1) * block, :], x[j * block:(j + 1) * block, :], NT,
                                      preferred_element_type=F32).astype(BF16)
                gram[i * block:(i + 1) * block, j * block:(j + 1) * block] = blk
                if j > i:
                    gram[j * block:(j + 1) * block, i * block:(i + 1) * block] = blk.T

    def polynomial():
        for i in range(nblk):
            ra, rb = i * block, (i + 1) * block
            strip = (COEF_B * gram[ra:rb, ra:].astype(F32) + COEF_C * dot(gram[ra:rb, :], gram[:, ra:])).astype(BF16)
            poly[ra:rb, ra:] = strip
            for j in range(i + 1, nblk):
                poly[j * block:(j + 1) * block, ra:rb] = strip[:, j * block - ra:(j + 1) * block - ra].T

    def update(lo, hi):
        @pl.loop(lo, hi)
        def _(t):
            cs = column(t)
            xc = x[:, cs]
            x[:, cs] = (COEF_A * xc.astype(F32) + dot(poly[...], xc)).astype(BF16)

    def in_middle(fn):
        @pl.when(middle)
        def _():
            fn()

    def whole(core):
        gathers[core][1]()
        gathers[core][2]()
        in_middle(normalize)

    def poly_and_update():
        polynomial()
        update(0, 1)

    head = {
        HEAD: lambda: whole(0),
        HEAD + 1: lambda: in_middle(square),
        HEAD + 2: lambda: in_middle(poly_and_update),
        HEAD + 3: lambda: in_middle(lambda: update(1, 2)),
        HEAD + 4: lambda: in_middle(lambda: update(2, 3)),
        HEAD + 5: lambda: in_middle(lambda: update(3, TP)),
    }

    chip_sum(0)
    copy_y(0).start()
    chip_sum(1)
    copy_y(1).start()
    for k in range(npiece):
        load_me(k).start()
        load_mom(k).start()
    sent = 2
    for k in range(npiece):
        for j in range(sent, SENT[k]):
            chip_sum(j)
        update_piece(k)
        for j in range(sent, SENT[k]):
            copy_y(j).start()
        sent = SENT[k]
        for (core, chip), todo in STAGES.items():
            if k in todo:
                @pl.when(jnp.logical_and(c == core, y == chip))
                def _():
                    for t in todo[k]:
                        gathers[core][0](t)
        if k in head:
            on_core(0, head[k])

    def copy_w(i):
        return mesh_copy(weight.at[peers[i]], wg.at[i - 1], pw, rw.at[i], dp=peers[i])

    wv = own_me
    load_w = [pltpu.make_async_copy(weight.at[peers[i]], wv.at[i], lw.at[i]) for i in range(DP)]
    for i in range(1, DP):
        copy_w(i).start()
    for cp in load_w:
        cp.start()

    on_core(1, lambda: whole(1))

    @pl.when(middle)
    def _():
        def step(i, carry):
            square()
            polynomial()

            @pl.when(i < NS_STEPS - 1)
            def _():
                update(0, TP)
            return carry
        lax.fori_loop(1 - c, NS_STEPS, step, 0)

    hrows = rows // 2

    def half_block(r, h):
        return pl.ds(pl.multiple_of(r * rows + h * hrows, hrows), hrows)

    def half(h):
        return pl.ds(h * hrows, hrows)

    def copy_e(i, h):
        blk = half_block(peers[i], h)
        return mesh_copy(x5e.at[blk, :], x5.at[blk, :], se, re.at[i, h], tp=end)

    def last(i, s, dst):
        blk = row_block(peers[i])
        dst[blk, :] = (COEF_A * x[blk, column(s)].astype(F32) + dot(poly[blk, :], x[:, column(s)])).astype(BF16)

    def apply(w, v, mat):
        return w - lr[mat] * (out_scale * v.astype(F32) + decay[0] * w)

    def each(h, fn):
        @pl.loop(0, hrows // STEP)
        def _(i):
            fn(pl.multiple_of(h * hrows + i * STEP, STEP))

    def to_partner(src, mat, r, h, sem, slot):
        return mesh_copy(src, wb.at[mat, half_block(r, h), :], sem, rd.at[slot, h], dp=partner)

    def send_x(i, h):
        return mesh_copy(x5.at[half_block(peers[i], h), :], xr.at[me, half(h), :], sx, rx.at[me, h], dp=peers[i])

    def send_w(i, h):
        return mesh_copy(ws.at[i, half(h), :], wb.at[me, half_block(peers[i], h), :], sw, rwb.at[me, h], dp=peers[2 + i])

    def share_own(i, h):
        return to_partner(ws.at[i, half(h), :], me, peers[i], h, sd, (0, None, 1, 2)[i])

    def share_mine(i, h):
        return to_partner(wo.at[i, half(h), :], peers[i], me, h, sm2, 1 + i)

    def pass_on(i, h):
        return to_partner(wb.at[peers[i], half_block(yp, h), :], peers[i], yp, h, sf, 3 + i)

    def store_b(i, h):
        return pltpu.make_async_copy(ws.at[i, half(h), :], wb.at[me, half_block(peers[i], h), :], sl_b)

    def store_o(i, h):
        return pltpu.make_async_copy(wo.at[i, half(h), :], wb.at[peers[i], half_block(me, h), :], sl_o)

    def store_n(i, h):
        return pltpu.make_async_copy(wv.at[i, half(h), :], w_new.at[peers[i], half(h), :], sl_n)

    halves = (0, 1)

    for i in (2, 3, 0, 1):
        r = peers[i]

        @pl.when(middle)
        def _():
            last(i, end, x5e)
            for h in halves:
                copy_e(i, h).start()
            last(i, z, x5)

        if i == 0:
            load_w[0].wait()
        else:
            copy_w(i).wait_recv()
        for h in halves:
            @pl.when(jnp.logical_not(middle))
            def _():
                copy_e(i, h).wait_recv()

            if i > 0:
                send_x(i, h).start()

            def rows_of(lo, i=i, r=r):
                sl = pl.ds(lo, STEP)
                v = x5[pl.ds(pl.multiple_of(r * rows + lo, STEP), STEP), :]
                if i == 0:
                    w = apply(wv[0, sl, :], v, me)
                    wv[0, sl, :] = w
                else:
                    w = apply(wg[i - 1, sl, :], v, me)
                ws[i, sl, :] = w.astype(BF16)
            each(h, rows_of)
            if i < 2:
                send_w(i, h).start()
            if i != 1:
                share_own(i, h).start()
            store_b(i, h).start()
            if i == 0:
                store_n(0, h).start()

    def mine(i):
        mat = peers[i]
        load_w[i].wait()
        for h in halves:
            mesh_copy(x5.at[half_block(me, h), :], xr.at[mat, half(h), :], sx, rx.at[mat, h], dp=mat).wait_recv()

            def rows_of(lo):
                sl = pl.ds(lo, STEP)
                w = apply(wv[i, sl, :], xr[mat, sl, :], mat)
                wv[i, sl, :] = w
                wo[i, sl, :] = w.astype(BF16)
            each(h, rows_of)
            if i > 1:
                share_mine(i, h).start()
            store_n(i, h).start()
            store_o(i, h).start()

    def relay(i):
        for h in halves:
            mesh_copy(ws.at[0, half(h), :], wb.at[peers[i], half_block(yp, h), :], sw, rwb.at[peers[i], h],
                      dp=peers[i]).wait_recv()
            pass_on(i, h).start()

    def core0_order():
        mine(2)
        relay(2)
        mine(1)
        mine(3)
        relay(3)

    def core1_order():
        mine(1)
        mine(3)
        relay(3)
        mine(2)
        relay(2)

    mesh_copy(recv_a, recv_a, sa, ra.at[0], dp=partner).wait_send()
    mesh_copy(recv_b, recv_b, sb, rb, dp=partner).wait_send()
    mesh_copy(own_yp, own_yp, sy, ry.at[0], dp=yp).wait_send()
    pltpu.make_async_copy(momb, momb, sm).wait()
    mesh_copy(ub.at[1:DP], ub.at[1:DP], su, ru.at[0, 0], dp=partner).wait_send()
    mesh_copy(wg, wg, pw, rw.at[0], dp=partner).wait_send()

    on_core(0, core0_order)
    on_core(1, core1_order)

    arrivals = ((partner, partner), (partner, diag), (partner, yp), (diag, partner), (yp, partner), (diag, diag), (yp, diag))
    for slot, (mat, r) in enumerate(arrivals):
        for h in halves:
            to_partner(ws.at[0, half(h), :], mat, r, h, sd, slot).wait_recv()

    @pl.when(middle)
    def _():
        mesh_copy(x5e, x5e, se, re.at[0, 0], tp=end).wait_send()

    def sent(n, sem, slot):
        mesh_copy(ws.at[0:n], ws.at[0:n], sem, slot, dp=partner).wait_send()

    sent(3, sx, rx.at[0, 0])
    sent(2, sw, rwb.at[0, 0])
    sent(3, sd, rd.at[0, 0])
    sent(2, sm2, rd.at[0, 0])
    sent(2, sf, rd.at[0, 0])
    pltpu.make_async_copy(ws, ws, sl_b).wait()
    pltpu.make_async_copy(wo.at[1:DP], wo.at[1:DP], sl_o).wait()
    pltpu.make_async_copy(wv, wv, sl_n).wait()


def muon(grad, mom, weight, lr, decay, out_scale):
    _, mats, all_rows, cols = grad.shape
    rows = mom.shape[1]
    n = len(ORDER)
    nq = DP * MAX_PARTS
    dma = pltpu.SemaphoreType.DMA
    hbm = pl.BlockSpec(memory_space=pl.ANY)
    smem = pl.BlockSpec(memory_space=pltpu.SMEM)
    f32 = pltpu.VMEM((mats, rows, cols), F32)
    b16 = pltpu.VMEM((mats, rows, cols), BF16)
    square = pltpu.VMEM((all_rows, all_rows), BF16)
    slab = pltpu.VMEM((all_rows, cols), BF16)
    return pl.pallas_call(
        functools.partial(muon_kernel, out_scale),
        out_shape=(jax.ShapeDtypeStruct(mom.shape, F32), jax.ShapeDtypeStruct(weight.shape, F32),
                   jax.ShapeDtypeStruct((mats, all_rows, cols), BF16)),
        in_specs=[hbm] * 3 + [smem] * 2,
        out_specs=[hbm] * 3,
        scratch_shapes=[f32] * 6 + [b16, pltpu.VMEM((all_rows, TP * cols), BF16), square, square, slab, slab,
                                    pltpu.VMEM((DP - 1, rows, cols), F32), b16, b16, b16, pltpu.VMEM((16, TP * cols), F32)]
        + [dma((2,)), dma, dma, dma] + [dma((n,)), dma, dma, dma, dma((n,)), dma, dma, dma((DP, MAX_PARTS)), dma, dma, dma((3, nq)), dma, dma((DP,)),
           dma((DP,)), dma, dma((DP, 2)), dma, dma((DP, 2)), dma, dma((DP, 2))] + [dma] * 6 + [dma((7, 2))],
        compiler_params=pltpu.CompilerParams(collective_id=0, has_side_effects=True, vmem_limit_bytes=67043328),
        name="muon",
    )(grad, mom, weight, lr, decay)


def copy_kernel(*refs):
    n = len(refs) // 4
    sources, outs, bufs, sems = refs[:n], refs[n:2 * n], refs[2 * n:3 * n], refs[3 * n:]
    reads, writes = [], []
    for src, out, buf, sem in zip(sources, outs, bufs, sems):
        for i in range(src.shape[0]):
            reads.append(pltpu.make_async_copy(src.at[i], buf.at[i], sem.at[0, i]))
            writes.append(pltpu.make_async_copy(buf.at[i], out.at[i], sem.at[1, i]))
    for cp in reads:
        cp.start()
    for rd, wr in zip(reads, writes):
        rd.wait()
        wr.start()
    for cp in writes:
        cp.wait()


def results(*arrays):
    flat = [v.reshape(-1, 256, v.shape[-1]) for v in arrays]
    hbm = pl.BlockSpec(memory_space=pl.ANY)
    out = pl.pallas_call(
        copy_kernel,
        out_shape=tuple(jax.ShapeDtypeStruct(v.shape, v.dtype) for v in flat),
        in_specs=[hbm] * len(flat),
        out_specs=(hbm,) * len(flat),
        scratch_shapes=[pltpu.VMEM(v.shape, v.dtype) for v in flat]
        + [pltpu.SemaphoreType.DMA((2, v.shape[0])) for v in flat],
        compiler_params=pltpu.CompilerParams(vmem_limit_bytes=67043328),
        name="results",
    )(*flat)
    return tuple(o.reshape(v.shape) for o, v in zip(out, arrays))


def solution(mesh):
    def local_step(grad, mom, weight, learn_rate, decay_rate):
        out_scale = 0.2 * math.sqrt(max(grad.shape[2], grad.shape[3] * TP))
        return results(*muon(grad, mom, weight, learn_rate, decay_rate.reshape(1), out_scale))

    return jax.shard_map(
        local_step,
        mesh=mesh,
        in_specs=(P(("rep", "dp"), None, None, "tp"), P("rep", "dp", "tp"), P("rep", "dp", "tp"), P("rep"), P()),
        out_specs=(P("rep", "dp", "tp"), P("rep", "dp", "tp"), P("rep", None, "tp")),
        check_vma=False,
    )
```
